128 devices in a mesh: inst: 1, dev: 64 (over z, y, x), side: 2 (over core).
Axes of the slice: x: 4, y: 4, z: 4, core: 2. Of those that a mesh axis runs over, the one named last changes fastest.
Arguments:
- hidden: bfloat16 [512, 3072], P(('inst', 'dev'))
- cache_len: int32 [512], P(('inst', 'dev'))
- k_cache: bfloat16 [1, 512, 8, 256, 128], P(None, ('inst', 'dev'))
- v_cache: bfloat16 [1, 512, 8, 256, 128], P(None, ('inst', 'dev'))
- w_q: bfloat16 [1, 3072, 3072], replicated
- w_kv: bfloat16 [1, 3072, 2048], replicated
- w_o: bfloat16 [1, 3072, 3072], replicated
- attn_gain: float32 [1, 3072], replicated
- ffn_gain: float32 [1, 3072], replicated
- w_gate: bfloat16 [1, 3072, 8192], P(None, None, 'dev')
- w_up: bfloat16 [1, 3072, 8192], P(None, None, 'dev')
- w_down: bfloat16 [1, 8192, 3072], P(None, 'dev')
Outputs:
- output: bfloat16 [512, 3072], P(('inst', 'dev', 'side'))
All inputs are finite; a program needn't handle non-finite values.
Results may differ from the reference program's by a relative error of at most 0.0121802.
Values are sent between devices in bfloat16 or wider.
A program may use at most 1 GiB of HBM per device.

```python
import math
import jax
import jax.numpy as jnp
from jax import lax

D = 3072
FF = 8192
HEADS = 24
KV_HEADS = 8
HEAD = 128
SEQ = 256
LAYERS = 1
BATCH = 512

EPS = 1e-5
ROPE_BASE = 10000.0
KEY_STD = math.sqrt(1.5 * math.log(SEQ))
GROUP = HEADS // KV_HEADS


def setup_inputs(seed: int = 0, part: int = 0) -> dict:
    base_key = jax.random.key(seed)
    part_key = jax.random.fold_in(base_key, part)
    shared = jax.random.split(base_key, 8)
    local = jax.random.split(part_key, 6)
    hidden = jax.random.normal(local[0], (BATCH, D), jnp.float32)
    cache_len = jax.random.randint(local[1], (BATCH,), 1, SEQ + 1, dtype=jnp.int32)
    cache_len = cache_len.at[0].set(SEQ).at[1].set(1)
    cache_shape = (LAYERS, BATCH, KV_HEADS, SEQ, HEAD)
    mean_shape = (LAYERS, BATCH, KV_HEADS, 1, HEAD)
    pos_ramp = (2.0 * jnp.arange(SEQ, dtype=jnp.float32) / SEQ - 1.0).reshape(1, 1, 1, SEQ, 1)
    k_cache = KEY_STD * jax.random.normal(local[2], cache_shape, jnp.float32)
    v_cache = (jax.random.normal(local[3], cache_shape, jnp.float32)
               + 0.7 * jax.random.normal(local[4], mean_shape, jnp.float32)
               + 0.7 * pos_ramp * jax.random.normal(local[5], mean_shape, jnp.float32))
    kv_cols = KV_HEADS * HEAD
    col_scale = jnp.concatenate([jnp.full((kv_cols,), KEY_STD, jnp.float32), jnp.full((kv_cols,), 2.0, jnp.float32)])
    w_q = jax.random.normal(shared[0], (LAYERS, D, HEADS * HEAD), jnp.float32) * D ** -0.5
    w_kv = jax.random.normal(shared[1], (LAYERS, D, 2 * kv_cols), jnp.float32) * (D ** -0.5) * col_scale
    w_o = jax.random.normal(shared[2], (LAYERS, HEADS * HEAD, D), jnp.float32) * (HEADS * HEAD) ** -0.5
    attn_gain = jax.random.uniform(shared[3], (LAYERS, D), jnp.float32, 0.5, 1.5)
    ffn_gain = jax.random.uniform(shared[4], (LAYERS, D), jnp.float32, 0.5, 1.5)
    w_gate = jax.random.normal(shared[5], (LAYERS, D, FF), jnp.float32) * D ** -0.5
    w_up = jax.random.normal(shared[6], (LAYERS, D, FF), jnp.float32) * D ** -0.5
    w_down = jax.random.normal(shared[7], (LAYERS, FF, D), jnp.float32) * (1.5 * FF ** -0.5)
    return {
        'hidden': hidden.astype(jnp.bfloat16),
        'cache_len': cache_len,
        'k_cache': k_cache.astype(jnp.bfloat16),
        'v_cache': v_cache.astype(jnp.bfloat16),
        'w_q': w_q.astype(jnp.bfloat16),
        'w_kv': w_kv.astype(jnp.bfloat16),
        'w_o': w_o.astype(jnp.bfloat16),
        'attn_gain': attn_gain,
        'ffn_gain': ffn_gain,
        'w_gate': w_gate.astype(jnp.bfloat16),
        'w_up': w_up.astype(jnp.bfloat16),
        'w_down': w_down.astype(jnp.bfloat16),
    }


def rms_norm(rows, gain):
    rows_f = rows.astype(jnp.float32)
    inv_rms = lax.rsqrt(jnp.mean(rows_f * rows_f, axis=-1, keepdims=True) + EPS)
    return (rows_f * inv_rms * gain).astype(jnp.bfloat16)


def rotary(vecs, positions):
    half_dim = vecs.shape[-1] // 2
    freqs = ROPE_BASE ** (-jnp.arange(half_dim, dtype=jnp.float32) / half_dim)
    angle = positions.astype(jnp.float32)[:, None, None] * freqs
    cos_part = jnp.cos(angle)
    sin_part = jnp.sin(angle)
    first = vecs[..., :half_dim]
    second = vecs[..., half_dim:]
    return jnp.concatenate([first * cos_part - second * sin_part, second * cos_part + first * sin_part], axis=-1)


def attend_one(operands):
    q_row, k_new, v_new, k_seq, v_seq, length = operands
    scale = HEAD ** -0.5
    q_f = q_row.astype(jnp.float32)
    scores = jnp.einsum('kgd,ksd->kgs', q_f, k_seq.astype(jnp.float32)) * scale
    valid = jnp.arange(SEQ)[None, None, :] < length
    scores = jnp.where(valid, scores, -1e30)
    self_score = jnp.einsum('kgd,kd->kg', q_f, k_new.astype(jnp.float32)) * scale
    row_max = jnp.maximum(jnp.max(scores, axis=-1), self_score)
    exp_scores = jnp.exp(scores - row_max[..., None])
    self_exp = jnp.exp(self_score - row_max)
    total_exp = jnp.sum(exp_scores, axis=-1) + self_exp
    mixed = jnp.einsum('kgs,ksd->kgd', exp_scores.astype(jnp.bfloat16).astype(jnp.float32), v_seq.astype(jnp.float32))
    mixed = mixed + self_exp.astype(jnp.bfloat16).astype(jnp.float32)[..., None] * v_new.astype(jnp.float32)[:, None, :]
    return (mixed / total_exp[..., None]).astype(jnp.bfloat16)


def reference(hidden, cache_len, k_cache, v_cache, w_q, w_kv, w_o, attn_gain, ffn_gain, w_gate, w_up, w_down):
    def layer_step(x_cur, per_layer):
        q_weight, kv_weight, o_weight, gain_attn, gain_ffn, gate_weight, up_weight, down_weight, k_layer, v_layer = per_layer
        normed = rms_norm(x_cur, gain_attn)
        q_all = jnp.dot(normed, q_weight, preferred_element_type=jnp.float32).reshape(BATCH, HEADS, HEAD)
        kv_all = jnp.dot(normed, kv_weight, preferred_element_type=jnp.float32).reshape(BATCH, 2, KV_HEADS, HEAD)
        q_rows = rotary(q_all, cache_len).astype(jnp.bfloat16).reshape(BATCH, KV_HEADS, GROUP, HEAD)
        k_new = rotary(kv_all[:, 0], cache_len).astype(jnp.bfloat16)
        v_new = kv_all[:, 1].astype(jnp.bfloat16)
        mixed = lax.map(attend_one, (q_rows, k_new, v_new, k_layer, v_layer, cache_len))
        attn_out = jnp.dot(mixed.reshape(BATCH, HEADS * HEAD), o_weight, preferred_element_type=jnp.float32)
        x_mid = (x_cur.astype(jnp.float32) + attn_out).astype(jnp.bfloat16)
        h_rows = rms_norm(x_mid, gain_ffn)
        gate = jnp.dot(h_rows, gate_weight, preferred_element_type=jnp.float32)
        up_proj = jnp.dot(h_rows, up_weight, preferred_element_type=jnp.float32)
        act_rows = (jax.nn.silu(gate) * up_proj).astype(jnp.bfloat16)
        y_rows = jnp.dot(act_rows, down_weight, preferred_element_type=jnp.float32).astype(jnp.bfloat16)
        x_next = (x_mid.astype(jnp.float32) + y_rows.astype(jnp.float32)).astype(jnp.bfloat16)
        return x_next, None

    x_out, _ = lax.scan(layer_step, hidden, (w_q, w_kv, w_o, attn_gain, ffn_gain, w_gate, w_up, w_down, k_cache, v_cache))
    return x_out
```

```python
import numpy as np
import jax
import jax.numpy as jnp
from jax import lax
from jax.experimental import pallas as pl
from jax.experimental.pallas import tpu as pltpu
from jax.sharding import PartitionSpec as P

EPS = 1e-5
ROPE_BASE = 10000.0
MESH = pl.DeviceIdType.MESH
F32 = jnp.float32
BF16 = jnp.bfloat16

N_DEV = 64
D = 3072
DH = D // 2
PART = 512
FFC = 128
SEQ = 256
HEAD = 128
KVH = 4
GROUP = 3
GRP = 8
NC = D // GRP
ROWS = 256


def coords(dev):
    return dev % 4, (dev // 4) % 4, dev // 16


def flat(x, y, z):
    return z * 16 + y * 4 + x


def ring_slot(part, dev):
    x, y, z = coords(dev)
    if part == 0:
        return x, z * 4 + y
    if part == 1:
        return y, z * 4 + x
    return z, y * 4 + x


def chip_at(part, ring, plane):
    if part == 0:
        return flat(ring, plane % 4, plane // 4)
    if part == 1:
        return flat(plane % 4, ring, plane // 4)
    return flat(plane % 4, plane // 4, ring)


def body(lens, hid, again, fgain, freq, kc, vc, wq, wkv, wo, wg, wu, wd, out,
         wq_b, wkv_b, wo_b, kc_b, vc_b, wgu_b, wd_b, a_b, kv_b, o_b, p_own, p_oth, x1f,
         hbuf, h2, gu_o, gu_m, gu_r, ubuf, y2, ysend, yrecv, tab, lens_v,
         w_sem, kv_sem, c_sem, wo_sem, f_sem, wd_sem, wds_sem, wdr_sem,
         ps_sem, pr_sem, a1s, a1r, a2s, a2r, gs_sem, gr_sem, us_sem, ur_sem, ys_sem, yr_sem):
    dev = lax.axis_index("dev")
    side = lax.axis_index("side")
    me = dev * 2 + side
    cx, cy, cz = coords(dev)
    j_me = (cx % 2) + 2 * (cy % 2) + 4 * (cz % 2)
    other = 1 - side

    def kv_copy(i):
        col = pl.multiple_of(i * 1024 + side * 512, 128)
        return pltpu.make_async_copy(wkv.at[0, :, pl.ds(col, 512)], wkv_b.at[i], kv_sem.at[i])

    def q_copy(h):
        col = pl.multiple_of(side * DH + h * 384, 128)
        return pltpu.make_async_copy(wq.at[0, :, pl.ds(col, 384)], wq_b.at[h], w_sem.at[h])

    def c_copy(i):
        src, dst = (kc, kc_b) if i == 0 else (vc, vc_b)
        return pltpu.make_async_copy(src.at[0, :, pl.ds(side * KVH, KVH)], dst, c_sem.at[i])

    def o_copy(n):
        row = pl.multiple_of(side * DH, 128)
        return pltpu.make_async_copy(wo.at[0, pl.ds(row, DH), pl.ds(pl.multiple_of(n * 512, 128), 512)], wo_b.at[n], wo_sem.at[n])

    def f_copy(i):
        row = pl.multiple_of(side * DH, 128)
        src = wg if i == 0 else wu
        return pltpu.make_async_copy(src.at[0, pl.ds(row, DH), :], wgu_b.at[:, pl.ds(i * FFC, FFC)], f_sem.at[i])

    wd_own = pltpu.make_async_copy(wd.at[0, :, pl.ds(pl.multiple_of(j_me * NC, 128), NC)], wd_b.at[j_me], wd_sem)

    kv_copy(0).start()
    kv_copy(1).start()
    q_copy(0).start()
    c_copy(0).start()
    c_copy(1).start()
    for h in range(1, KVH):
        q_copy(h).start()
    for n in range(6):
        o_copy(n).start()
    f_copy(0).start()
    f_copy(1).start()
    wd_own.start()

    barrier = pltpu.get_barrier_semaphore()

    def greet(i, c):
        t = (me + i) % (2 * N_DEV)
        pl.semaphore_signal(barrier, inc=1, device_id=(0, t // 2, t % 2), device_id_type=MESH)
        return c

    lax.fori_loop(1, 2 * N_DEV, greet, 0)

    rowb = lax.broadcasted_iota(jnp.int32, (8, 128), 0)
    lv = jnp.zeros((8, 128), jnp.int32)
    for b in range(8):
        lv = jnp.where(rowb == b, lens[b], lv)
    angle = lv.astype(F32) * freq[...]
    lane = lax.broadcasted_iota(jnp.int32, (8, 128), 1)
    sin = jnp.sin(angle)
    tab[0] = jnp.cos(angle)
    tab[1] = jnp.where(lane < 64, -sin, sin)
    lens_v[...] = jnp.concatenate([lv, lv, lv], axis=0)

    def rotary(v):
        return v * tab[0] + pltpu.roll(v, 64, axis=1) * tab[1]

    xf = hid[...].astype(F32)
    inv = lax.rsqrt(jnp.mean(xf * xf, axis=-1, keepdims=True) + EPS)
    a_b[...] = (xf * inv * again[...]).astype(BF16)

    for i in range(2):
        kv_copy(i).wait()
        kv = jnp.dot(a_b[...], wkv_b[i], preferred_element_type=F32)
        for h in range(KVH):
            v = kv[:, h * HEAD:(h + 1) * HEAD]
            if i == 0:
                v = rotary(v)
            kv_b[i, h] = v.astype(BF16).astype(F32)

    pl.semaphore_wait(barrier, 2 * N_DEV - 1)

    def block_peer(k):
        px = cx + (k % 2) * (1 - 2 * (cx % 2))
        py = cy + ((k // 2) % 2) * (1 - 2 * (cy % 2))
        pz = cz + (k // 4) * (1 - 2 * (cz % 2))
        return flat(px, py, pz), (px % 2) + 2 * (py % 2) + 4 * (pz % 2)

    def wd_copy(k):
        peer, j = block_peer(k)
        return pltpu.make_async_remote_copy(
            src_ref=wd.at[0, :, pl.ds(pl.multiple_of(j * NC, 128), NC)], dst_ref=wd_b.at[j_me],
            send_sem=wds_sem.at[k], recv_sem=wdr_sem.at[k], device_id=(0, peer, side), device_id_type=MESH)

    for k in range(1, GRP):
        wd_copy(k).start()

    rowm = lax.broadcasted_iota(jnp.int32, (24, SEQ), 0) % 8
    rowv = lax.broadcasted_iota(jnp.int32, (24, HEAD), 0) % 8
    pos = lax.broadcasted_iota(jnp.int32, (24, SEQ), 1)
    scale = HEAD ** -0.5
    c_copy(0).wait()
    c_copy(1).wait()

    def attend(h, c):
        q_copy(h).wait()
        q = jnp.dot(a_b[...], wq_b[h], preferred_element_type=F32)
        qf = jnp.concatenate([rotary(q[:, g * HEAD:(g + 1) * HEAD]) for g in range(GROUP)], axis=0)
        qb = qf.astype(BF16)
        k_new = kv_b[0, h]
        v_new = kv_b[1, h]
        k3 = jnp.concatenate([k_new, k_new, k_new], axis=0)
        v3 = jnp.concatenate([v_new, v_new, v_new], axis=0)
        self_score = jnp.sum(qb.astype(F32) * k3, axis=-1, keepdims=True) * scale
        s = jnp.zeros((24, SEQ), F32)
        for b in range(8):
            sb = lax.dot_general(qb, kc_b[b, h], (((1,), (1,)), ((), ())), preferred_element_type=F32)
            s = jnp.where(rowm == b, sb, s)
        limit = lens_v[...]
        limit = jnp.concatenate([limit, limit], axis=1)
        s = jnp.where(pos < limit, s * scale, -1e30)
        top = jnp.maximum(jnp.max(s, axis=-1, keepdims=True), self_score)
        e = jnp.exp(s - top)
        es = jnp.exp(self_score - top)
        total = jnp.sum(e, axis=-1, keepdims=True) + es
        eb = e.astype(BF16)
        m = jnp.zeros((24, HEAD), F32)
        for b in range(8):
            mb = jnp.dot(eb, vc_b[b, h], preferred_element_type=F32)
            m = jnp.where(rowv == b, mb, m)
        m = m + es.astype(BF16).astype(F32) * v3
        o = m / total
        for g in range(GROUP):
            o_b[h, :, g * HEAD:(g + 1) * HEAD] = o[g * 8:(g + 1) * 8].astype(BF16)
        return c

    lax.fori_loop(0, KVH, attend, 0)

    def p_copy(n):
        return pltpu.make_async_remote_copy(
            src_ref=p_own.at[n], dst_ref=p_oth.at[n], send_sem=ps_sem.at[n], recv_sem=pr_sem.at[n],
            device_id=(0, dev, other), device_id_type=MESH)

    o_all = jnp.concatenate([o_b[h] for h in range(KVH)], axis=1)

    def project(n, c):
        o_copy(n).wait()
        p_own[n] = jnp.dot(o_all, wo_b[n], preferred_element_type=F32)
        p_copy(n).start()
        return c

    lax.fori_loop(0, 6, project, 0)

    ssq = jnp.zeros((8, 1), F32)
    for n in range(6):
        p_copy(n).wait_recv()
        v = hid[:, n * 512:(n + 1) * 512].astype(F32) + (p_own[n] + p_oth[n])
        v = v.astype(BF16).astype(F32)
        x1f[n] = v
        ssq = ssq + jnp.sum(v * v, axis=-1, keepdims=True)
    inv1 = lax.rsqrt(ssq / D + EPS)

    for q in range(3):
        ring, plane = ring_slot(q, dev)
        v = x1f[side * 3 + q] * inv1 * fgain[side * 3 + q]
        hbuf[q, ring, plane] = v.astype(BF16)

    def a1_copy(q, k):
        ring, plane = ring_slot(q, dev)
        to = ((plane // 4 + k // 4) % 4) * 4 + (plane + k) % 4
        return pltpu.make_async_remote_copy(
            src_ref=hbuf.at[q, ring, plane], dst_ref=hbuf.at[q, ring, plane],
            send_sem=a1s.at[q], recv_sem=a1r.at[q],
            device_id=(0, chip_at(q, ring, to), side), device_id_type=MESH)

    def to_plane(k, c):
        for q in range(3):
            ring, plane = ring_slot(q, dev)
            to = ((plane // 4 + k // 4) % 4) * 4 + (plane % 4 + k % 4) % 4
            pltpu.make_async_remote_copy(
                src_ref=hbuf.at[q, ring, plane], dst_ref=hbuf.at[q, ring, plane],
                send_sem=a1s.at[q], recv_sem=a1r.at[q],
                device_id=(0, chip_at(q, ring, to), side), device_id_type=MESH).start()
        return c

    lax.fori_loop(1, 16, to_plane, 0)

    def a2_copy(q, k):
        ring, plane = ring_slot(q, dev)
        to = (ring + k) % 4
        return pltpu.make_async_remote_copy(
            src_ref=hbuf.at[q, ring], dst_ref=hbuf.at[q, ring],
            send_sem=a2s.at[q], recv_sem=a2r.at[q],
            device_id=(0, chip_at(q, to, plane), side), device_id_type=MESH)

    for q in range(3):
        pltpu.make_async_copy(hbuf.at[q, 0, pl.ds(0, 15)], hbuf.at[q, 0, pl.ds(0, 15)], a1r.at[q]).wait()
        for k in (1, 3, 2):
            a2_copy(q, k).start()
    for q in range(3):
        pltpu.make_async_copy(hbuf.at[q, pl.ds(0, 3)], hbuf.at[q, pl.ds(0, 3)], a2r.at[q]).wait()

    f_copy(0).wait()
    f_copy(1).wait()

    def arrange(half):
        def pair(i, c):
            for q in range(3):
                vs = []
                for t in range(2):
                    ring, plane = ring_slot(q, half * 32 + 2 * i + t)
                    vs.append(hbuf[q, ring, plane].astype(F32))
                h2[pl.ds(pl.multiple_of(i * 16, 16), 16), q * PART:(q + 1) * PART] = jnp.concatenate(vs, axis=0).astype(BF16)
            return c
        lax.fori_loop(0, 16, pair, 0)

    g_copy = pltpu.make_async_remote_copy(
        src_ref=gu_o, dst_ref=gu_r, send_sem=gs_sem, recv_sem=gr_sem, device_id=(0, dev, other), device_id_type=MESH)
    arrange(other)
    gu_o[...] = jnp.dot(h2[...], wgu_b[...], preferred_element_type=F32)
    g_copy.start()
    arrange(side)
    gu_m[...] = jnp.dot(h2[...], wgu_b[...], preferred_element_type=F32)
    g_copy.wait_recv()
    gate = gu_m[:, :FFC] + gu_r[:, :FFC]
    up = gu_m[:, FFC:] + gu_r[:, FFC:]
    ubuf[j_me] = (gate * jax.nn.sigmoid(gate) * up).astype(BF16)

    def u_copy(k):
        peer, _ = block_peer(k)
        return pltpu.make_async_remote_copy(
            src_ref=ubuf.at[j_me], dst_ref=ubuf.at[j_me], send_sem=us_sem.at[k], recv_sem=ur_sem.at[k],
            device_id=(0, peer, side), device_id_type=MESH)

    for k in range(1, GRP):
        u_copy(k).start()
    wd_own.wait()
    for k in range(1, GRP):
        wd_copy(k).wait_recv()
    for k in range(1, GRP):
        u_copy(k).wait_recv()
    u_all = jnp.concatenate([ubuf[j] for j in range(GRP)], axis=1)
    y2[...] = jnp.dot(u_all, wd_b[...].reshape(GRP * FFC, NC), preferred_element_type=F32)

    def cut(i, c):
        v = y2[pl.ds(pl.multiple_of(i * 8, 8), 8), :]
        ysend[2 * i] = v[0:4]
        ysend[2 * i + 1] = v[4:8]
        return c

    lax.fori_loop(0, 32, cut, 0)
    here = side == dev // 32

    def give(i, c):
        k = (i + me) % 64
        d = side * 32 + k // 2
        t = k % 2

        @pl.when(jnp.logical_or(d != dev, t != side))
        def _():
            pltpu.make_async_remote_copy(
                src_ref=ysend.at[k], dst_ref=yrecv.at[dev], send_sem=ys_sem, recv_sem=yr_sem,
                device_id=(0, d, t), device_id_type=MESH).start()
        return c

    lax.fori_loop(0, 64, give, 0)

    @pl.when(here)
    def _():
        yrecv[dev] = ysend[(dev % 32) * 2 + side]

    def wait_blocks(ref, sem):
        @pl.when(here)
        def _():
            pltpu.make_async_copy(ref.at[pl.ds(0, 63)], ref.at[pl.ds(0, 63)], sem).wait()

        @pl.when(jnp.logical_not(here))
        def _():
            pltpu.make_async_copy(ref, ref, sem).wait()

    wait_blocks(yrecv, yr_sem)
    x1 = jnp.concatenate([x1f[n] for n in range(6)], axis=1)
    x1 = jnp.where(side == 0, x1[0:4], x1[4:8])
    for j in range(GRP):
        acc = None
        for c in range(N_DEV):
            x, y, z = c % 4, (c // 4) % 4, c // 16
            if (x % 2) + 2 * (y % 2) + 4 * (z % 2) == j:
                acc = yrecv[c] if acc is None else acc + yrecv[c]
        out[:, j * NC:(j + 1) * NC] = (x1[:, j * NC:(j + 1) * NC] + acc.astype(BF16).astype(F32)).astype(BF16)

    for k in range(1, GRP):
        wd_copy(k).wait_send()
        u_copy(k).wait_send()
    for n in range(6):
        p_copy(n).wait_send()
    for q in range(3):
        pltpu.make_async_copy(hbuf.at[q, 0, pl.ds(0, 15)], hbuf.at[q, 0, pl.ds(0, 15)], a1s.at[q]).wait()
        pltpu.make_async_copy(hbuf.at[q, pl.ds(0, 3)], hbuf.at[q, pl.ds(0, 3)], a2s.at[q]).wait()
    g_copy.wait_send()
    wait_blocks(ysend, ys_sem)


def solution(mesh):
    batch_axes = ('inst', 'dev')
    in_specs = (
        P(batch_axes, None),
        P(batch_axes),
        P(None, batch_axes, None, None, None),
        P(None, batch_axes, None, None, None),
        P(), P(), P(), P(), P(),
        P(None, None, 'dev'),
        P(None, None, 'dev'),
        P(None, 'dev', None),
    )
    out_specs = P(('inst', 'dev', 'side'), None)
    half = HEAD // 2
    freqs = (ROPE_BASE ** (-np.arange(half, dtype=np.float64) / half)).astype(np.float32)
    freqs = np.concatenate([freqs, freqs])[None]

    def device_fn(hidden, cache_len, k_cache, v_cache, w_q, w_kv, w_o, attn_gain, ffn_gain, w_gate, w_up, w_down):
        vmem = pl.BlockSpec(memory_space=pltpu.VMEM)
        hbm = pl.BlockSpec(memory_space=pl.ANY)
        dma = pltpu.SemaphoreType.DMA
        return pl.pallas_call(
            body,
            out_shape=jax.ShapeDtypeStruct((4, D), BF16),
            in_specs=[pl.BlockSpec(memory_space=pltpu.SMEM)] + [vmem] * 4 + [hbm] * 8,
            out_specs=vmem,
            scratch_shapes=[
                pltpu.VMEM((KVH, D, 384), BF16),
                pltpu.VMEM((2, D, 512), BF16),
                pltpu.VMEM((6, DH, 512), BF16),
                pltpu.VMEM((8, KVH, SEQ, HEAD), BF16),
                pltpu.VMEM((8, KVH, SEQ, HEAD), BF16),
                pltpu.VMEM((DH, 2 * FFC), BF16),
                pltpu.VMEM((GRP, FFC, NC), BF16),
                pltpu.VMEM((8, D), BF16),
                pltpu.VMEM((2, KVH, 8, HEAD), F32),
                pltpu.VMEM((KVH, 8, 384), BF16),
                pltpu.VMEM((6, 8, 512), F32),
                pltpu.VMEM((6, 8, 512), F32),
                pltpu.VMEM((6, 8, 512), F32),
                pltpu.VMEM((3, 4, 16, 8, PART), BF16),
                pltpu.VMEM((ROWS, DH), BF16),
                pltpu.VMEM((ROWS, 2 * FFC), F32),
                pltpu.VMEM((ROWS, 2 * FFC), F32),
                pltpu.VMEM((ROWS, 2 * FFC), F32),
                pltpu.VMEM((GRP, ROWS, FFC), BF16),
                pltpu.VMEM((ROWS, NC), F32),
                pltpu.VMEM((64, 4, NC), F32),
                pltpu.VMEM((64, 4, NC), F32),
                pltpu.VMEM((2, 8, 128), F32),
                pltpu.VMEM((24, 128), jnp.int32),
                dma((KVH,)), dma((2,)), dma((2,)), dma((6,)), dma((2,)), dma, dma((GRP,)), dma((GRP,)),
                dma((6,)), dma((6,)), dma((3,)), dma((3,)), dma((3,)), dma((3,)), dma, dma,
                dma((GRP,)), dma((GRP,)), dma, dma,
            ],
            compiler_params=pltpu.CompilerParams(
                collective_id=0, has_side_effects=True, vmem_limit_bytes=60 * 1024 * 1024),
            name="decode_layer",
        )(cache_len, hidden, attn_gain, ffn_gain.reshape(6, 1, 512), jnp.asarray(freqs),
          k_cache, v_cache, w_q, w_kv, w_o, w_gate, w_up, w_down)

    return jax.shard_map(device_fn, mesh=mesh, in_specs=in_specs, out_specs=out_specs, check_vma=False)
```

```python
import numpy as np
import jax
import jax.numpy as jnp
from jax import lax
from jax.experimental import pallas as pl
from jax.experimental.pallas import tpu as pltpu
from jax.sharding import PartitionSpec as P

EPS = 1e-5
ROPE_BASE = 10000.0
MESH = pl.DeviceIdType.MESH
F32 = jnp.float32
BF16 = jnp.bfloat16

N_DEV = 64
D = 3072
DH = D // 2
PART = 512
FFC = 128
SEQ = 256
HEAD = 128
KVH = 4
GROUP = 3
GRP = 8
NC = D // GRP
ROWS = 256
CHUNKS = 4
CH = ROWS // CHUNKS
KVC = 768
ORDER = (0, 1, 3, 2)


def coords(dev):
    return dev % 4, (dev // 4) % 4, dev // 16


def flat(x, y, z):
    return z * 16 + y * 4 + x


def ring_slot(part, dev):
    x, y, z = coords(dev)
    if part == 0:
        return x, z * 4 + y
    if part == 1:
        return y, z * 4 + x
    return z, y * 4 + x


def chip_at(part, ring, plane):
    if part == 0:
        return flat(ring, plane % 4, plane // 4)
    if part == 1:
        return flat(plane % 4, ring, plane // 4)
    return flat(plane % 4, plane // 4, ring)


def body(lens, hid_h, again_h, fgain_h, freq_h, kc, vc, wq, wkv, wo, wg, wu, wd, out,
         hid, again, fgain, freq,
         wq_b, wkv_b, wo_b, kc_b, vc_b, wgu_b, wd_b, a_b, kv_b, o_b, p_own, p_oth, x1f,
         hbuf, h2, gu_o, gu_m, gu_r, ubuf, ysend, yrecv, tab, lens_v,
         i_sem, w_sem, kv_sem, c_sem, wo_sem, f_sem, wd_sem, wds_sem, wdr_sem,
         ps_sem, pr_sem, a1s, a1r, a2s, a2r, a2f, gs_sem, gr_sem, us_sem, ur_sem, ys_sem, yr_sem):
    dev = lax.axis_index("dev")
    side = lax.axis_index("side")
    me = dev * 2 + side
    cx, cy, cz = coords(dev)
    j_me = (cx + side) % 2 + 2 * ((cy + side) % 2) + 4 * ((cz + side) % 2)

    def turn(t):
        return ((cx + t) % 4) // 2 + 2 * (((cy + t) % 4) // 2)

    other = 1 - side

    def in_copy(i):
        src, dst = ((hid_h, hid), (again_h, again), (fgain_h, fgain), (freq_h, freq))[i]
        return pltpu.make_async_copy(src, dst, i_sem.at[i])

    def kv_copy(i, c):
        col = pl.multiple_of(i * 1024 + side * 512, 128)
        rows = pl.ds(c * KVC, KVC)
        return pltpu.make_async_copy(wkv.at[0, rows, pl.ds(col, 512)], wkv_b.at[i, rows], kv_sem.at[i, c])

    def q_copy(h):
        col = pl.multiple_of(side * DH + h * 384, 128)
        return pltpu.make_async_copy(wq.at[0, :, pl.ds(col, 384)], wq_b.at[h], w_sem.at[h])

    def c_copy(i, h):
        src, dst = (kc, kc_b) if i == 0 else (vc, vc_b)
        return pltpu.make_async_copy(src.at[0, :, side * KVH + h], dst.at[h], c_sem.at[i, h])

    def head_copies(h):
        q_copy(h).start()
        c_copy(0, h).start()
        c_copy(1, h).start()

    def o_copy(n):
        row = pl.multiple_of(side * DH, 128)
        return pltpu.make_async_copy(wo.at[0, pl.ds(row, DH), pl.ds(pl.multiple_of(n * 512, 128), 512)], wo_b.at[n], wo_sem.at[n])

    def f_copy(i):
        row = pl.multiple_of(side * DH, 128)
        src = wg if i == 0 else wu
        return pltpu.make_async_copy(src.at[0, pl.ds(row, DH), :], wgu_b.at[:, pl.ds(i * FFC, FFC)], f_sem.at[i])

    wd_own = pltpu.make_async_copy(wd.at[0, :, pl.ds(pl.multiple_of(j_me * NC, 128), NC)], wd_b.at[j_me], wd_sem)

    for i in range(4):
        in_copy(i).start()
    for c in range(D // KVC):
        kv_copy(0, c).start()
    for c in range(D // KVC):
        kv_copy(1, c).start()

    barrier = pltpu.get_barrier_semaphore()

    def pair(c):
        return (c + 1 + 2 * ((c + side) % 2)) % 4

    def block_peer(k):
        px = pair(cx) if k % 2 else cx
        py = pair(cy) if (k // 2) % 2 else cy
        pz = pair(cz) if k // 4 else cz
        return flat(px, py, pz), (px + side) % 2 + 2 * ((py + side) % 2) + 4 * ((pz + side) % 2)

    def greet(d, t):
        pl.semaphore_signal(barrier, inc=1, device_id=(0, d, t), device_id_type=MESH)

    with jax.named_scope("greet"):
        greet(dev, other)
        greet(block_peer(GRP - 1)[0], side)
        for i in range(1, 64):
            ix, iy, iz = coords(i)
            if not (ix and iy and iz):
                greet(flat((cx + ix) % 4, (cy + iy) % 4, (cz + iz) % 4), side)
    greeted = 38

    with jax.named_scope("inwait"):
        for i in range(4):
            in_copy(i).wait()

    with jax.named_scope("tables"):
        rowb = lax.broadcasted_iota(jnp.int32, (8, 128), 0)
        lv = jnp.zeros((8, 128), jnp.int32)
        for b in range(8):
            lv = jnp.where(rowb == b, lens[b], lv)
        angle = lv.astype(F32) * freq[...]
        lane = lax.broadcasted_iota(jnp.int32, (8, 128), 1)
        sin = jnp.sin(angle)
        tab[0] = jnp.cos(angle)
        tab[1] = jnp.where(lane < 64, -sin, sin)
        lens_v[...] = jnp.concatenate([lv, lv, lv], axis=0)

    def rotary(v):
        return v * tab[0] + pltpu.roll(v, 64, axis=1) * tab[1]

    with jax.named_scope("norm"):
        xf = hid[...].astype(F32)
        inv = lax.rsqrt(jnp.mean(xf * xf, axis=-1, keepdims=True) + EPS)
        a_b[...] = (xf * inv * again[...]).astype(BF16)

    for i in range(2):
        with jax.named_scope("kvwait"):
            for c in range(D // KVC):
                kv_copy(i, c).wait()
        head_copies(2 * i)
        head_copies(2 * i + 1)
        with jax.named_scope("kvdot"):
            kv = jnp.dot(a_b[...], wkv_b[i], preferred_element_type=F32)
            for h in range(KVH):
                v = kv[:, h * HEAD:(h + 1) * HEAD]
                if i == 0:
                    v = rotary(v)
                kv_b[i, h] = v.astype(BF16).astype(F32)

    rowm = lax.broadcasted_iota(jnp.int32, (24, SEQ), 0) % 8
    rowv = lax.broadcasted_iota(jnp.int32, (24, HEAD), 0) % 8
    pos = lax.broadcasted_iota(jnp.int32, (24, SEQ), 1)
    scale = HEAD ** -0.5

    def attend(h, c):
        with jax.named_scope("qwait"):
            q_copy(h).wait()

        @pl.when(h < 3)
        def _():
            o_copy(2 * h).start()
            o_copy(2 * h + 1).start()

        with jax.named_scope("qdot"):
            q = jnp.dot(a_b[...], wq_b[h], preferred_element_type=F32)
            qf = jnp.concatenate([rotary(q[:, g * HEAD:(g + 1) * HEAD]) for g in range(GROUP)], axis=0)
            qb = qf.astype(BF16)
        k_new = kv_b[0, h]
        v_new = kv_b[1, h]
        k3 = jnp.concatenate([k_new, k_new, k_new], axis=0)
        v3 = jnp.concatenate([v_new, v_new, v_new], axis=0)
        self_score = jnp.sum(qb.astype(F32) * k3, axis=-1, keepdims=True) * scale
        with jax.named_scope("cwait"):
            c_copy(0, h).wait()
            c_copy(1, h).wait()
        with jax.named_scope("mix"):
            s = jnp.zeros((24, SEQ), F32)
            for b in range(8):
                sb = lax.dot_general(qb, kc_b[h, b], (((1,), (1,)), ((), ())), preferred_element_type=F32)
                s = jnp.where(rowm == b, sb, s)
            limit = lens_v[...]
            limit = jnp.concatenate([limit, limit], axis=1)
            s = jnp.where(pos < limit, s * scale, -1e30)
            top = jnp.maximum(jnp.max(s, axis=-1, keepdims=True), self_score)
            e = jnp.exp(s - top)
            es = jnp.exp(self_score - top)
            total = jnp.sum(e, axis=-1, keepdims=True) + es
            eb = e.astype(BF16)
            m = jnp.zeros((24, HEAD), F32)
            for b in range(8):
                mb = jnp.dot(eb, vc_b[h, b], preferred_element_type=F32)
                m = jnp.where(rowv == b, mb, m)
            m = m + es.astype(BF16).astype(F32) * v3
            o = m / total
            for g in range(GROUP):
                o_b[h, :, g * HEAD:(g + 1) * HEAD] = o[g * 8:(g + 1) * 8].astype(BF16)
        return c

    lax.fori_loop(0, 2, attend, 0)
    with jax.named_scope("barrier"):
        pl.semaphore_wait(barrier, greeted)

    def wd_copy(k):
        peer, j = block_peer(k)
        return pltpu.make_async_remote_copy(
            src_ref=wd.at[0, :, pl.ds(pl.multiple_of(j * NC, 128), NC)], dst_ref=wd_b.at[j_me],
            send_sem=wds_sem.at[k], recv_sem=wdr_sem.at[k], device_id=(0, peer, side), device_id_type=MESH)

    with jax.named_scope("wdsend"):
        for k in range(1, GRP):
            wd_copy(k).start()

    lax.fori_loop(2, KVH, attend, 0)

    f_copy(0).start()
    f_copy(1).start()
    wd_own.start()

    def p_copy(n):
        return pltpu.make_async_remote_copy(
            src_ref=p_own.at[n], dst_ref=p_oth.at[n], send_sem=ps_sem.at[n], recv_sem=pr_sem.at[n],
            device_id=(0, dev, other), device_id_type=MESH)

    o_all = jnp.concatenate([o_b[h] for h in range(KVH)], axis=1)

    def project(n, c):
        o_copy(n).wait()
        p_own[n] = jnp.dot(o_all, wo_b[n], preferred_element_type=F32)
        p_copy(n).start()
        return c

    with jax.named_scope("project"):
        lax.fori_loop(0, 6, project, 0)

    with jax.named_scope("x1"):
        ssq = jnp.zeros((8, 1), F32)
        for n in range(6):
            p_copy(n).wait_recv()
            v = hid[:, n * 512:(n + 1) * 512].astype(F32) + (p_own[n] + p_oth[n])
            v = v.astype(BF16).astype(F32)
            x1f[n] = v
            ssq = ssq + jnp.sum(v * v, axis=-1, keepdims=True)
        inv1 = lax.rsqrt(ssq / D + EPS)

        at = []
        for q in range(3):
            ring, plane = ring_slot(q, dev)
            row, col = plane // 4, plane % 4
            at.append((ring, row, col))
            v = x1f[side * 3 + q] * inv1 * fgain[side * 3 + q]
            hbuf[q, ring, row, col] = v.astype(BF16)

    with jax.named_scope("ag1send"):
        for i in ORDER:
            for j in ORDER:
                if i or j:
                    for q in range(3):
                        ring, row, col = at[q]
                        to = ((row + i) % 4) * 4 + (col + j) % 4
                        pltpu.make_async_remote_copy(
                            src_ref=hbuf.at[q, ring, row, col], dst_ref=hbuf.at[q, ring, row, col],
                            send_sem=a1s.at[q], recv_sem=a1r.at[q, (4 - i) % 4],
                            device_id=(0, chip_at(q, ring, to), side), device_id_type=MESH).start()

    def a2_copy(q, g, step, src, sem):
        ring, row, col = at[q]
        part = hbuf.at[q, src, (row + ORDER[g]) % 4]
        return pltpu.make_async_remote_copy(
            src_ref=part, dst_ref=part, send_sem=a2s.at[q], recv_sem=sem,
            device_id=(0, chip_at(q, (ring + step) % 4, row * 4 + col), side), device_id_type=MESH)

    def own_row(g):
        for q in range(3):
            n = 3 if g == 0 else 4
            some = hbuf.at[q, 0, 0, pl.ds(0, n)]
            pltpu.make_async_copy(some, some, a1r.at[q, ORDER[g]]).wait()
            ring = at[q][0]
            a2_copy(q, g, 1, ring, a2r.at[q, 0, g]).start()
            a2_copy(q, g, 3, ring, a2r.at[q, 1, g]).start()

    def recv_row(q, sem):
        some = hbuf.at[q, 0, 0]
        pltpu.make_async_copy(some, some, sem).wait()

    def pass_row(g):
        for q in range(3):
            ring = at[q][0]
            if g in (0, 3):
                recv_row(q, a2r.at[q, 0, g])
                a2_copy(q, g, 1, (ring + 3) % 4, a2f.at[q, g]).start()
            else:
                recv_row(q, a2r.at[q, 1, g])
                a2_copy(q, g, 3, (ring + 1) % 4, a2f.at[q, g]).start()

    for step, g in ((own_row, 0), (own_row, 1), (own_row, 2), (own_row, 3), (pass_row, 0), (pass_row, 1), (pass_row, 2), (pass_row, 3)):
        with jax.named_scope(f"{step.__name__}{g}"):
            step(g)
    with jax.named_scope("ag2wait"):
        for g in range(4):
            for q in range(3):
                recv_row(q, a2r.at[q, 1 if g in (0, 3) else 0, g])
        for g in range(4):
            for q in range(3):
                recv_row(q, a2f.at[q, g])

    f_copy(0).wait()
    f_copy(1).wait()

    def arrange(half, r):
        first = half * 32 + ((r + turn(half)) % CHUNKS) * (32 // CHUNKS)
        for i in range(16 // CHUNKS):
            slots = [[ring_slot(q, first + 2 * i + t) for t in range(2)] for q in range(3)]
            for q in range(3):
                vs = [hbuf[q, ring, plane // 4, plane % 4].astype(F32) for ring, plane in slots[q]]
                h2[r % 2, i * 16:(i + 1) * 16, q * PART:(q + 1) * PART] = jnp.concatenate(vs, axis=0).astype(BF16)
        return h2[r % 2]

    def g_copy(r):
        return pltpu.make_async_remote_copy(
            src_ref=gu_o.at[r], dst_ref=gu_r.at[r], send_sem=gs_sem.at[r], recv_sem=gr_sem.at[r],
            device_id=(0, dev, other), device_id_type=MESH)

    def u_copy(k, r):
        peer, _ = block_peer(k)
        return pltpu.make_async_remote_copy(
            src_ref=ubuf.at[j_me, r], dst_ref=ubuf.at[j_me, r], send_sem=us_sem.at[k, r], recv_sem=ur_sem.at[k, r],
            device_id=(0, peer, side), device_id_type=MESH)

    for r in range(CHUNKS + 1):
        if r < CHUNKS:
            with jax.named_scope("gateup"):
                gu_o[r] = jnp.dot(arrange(other, r), wgu_b[...], preferred_element_type=F32)
                g_copy(r).start()
                gu_m[r] = jnp.dot(arrange(side, r), wgu_b[...], preferred_element_type=F32)
        if r >= 1:
            with jax.named_scope("uact"):
                g_copy(r - 1).wait_recv()
                both = gu_m[r - 1] + gu_r[r - 1]
                gate = both[:, :FFC]
                up = both[:, FFC:]
                ubuf[j_me, r - 1] = (gate * jax.nn.sigmoid(gate) * up).astype(BF16)
                for k in range(1, GRP):
                    u_copy(k, r - 1).start()

    wd_own.wait()
    with jax.named_scope("wdwait"):
        for k in range(1, GRP):
            wd_copy(k).wait_recv()

    here = side == dev // 32
    per = 64 // CHUNKS

    def finish(r, c):
        with jax.named_scope("uwait"):
            for k in range(1, GRP):
                u_copy(k, r).wait_recv()
        with jax.named_scope("down"):
            u_all = jnp.concatenate([ubuf[j, r] for j in range(GRP)], axis=1)
            y = jnp.dot(u_all, wd_b[...].reshape(GRP * FFC, NC), preferred_element_type=F32)
            base = ((r + turn(side)) % CHUNKS) * per
            for i in range(per // 2):
                ysend[base + 2 * i] = y[i * 8:i * 8 + 4]
                ysend[base + 2 * i + 1] = y[i * 8 + 4:i * 8 + 8]

        def give(i, c):
            k = base + (i + me) % per
            d = side * 32 + k // 2
            t = k % 2

            @pl.when(jnp.logical_or(d != dev, t != side))
            def _():
                pltpu.make_async_remote_copy(
                    src_ref=ysend.at[k], dst_ref=yrecv.at[dev], send_sem=ys_sem, recv_sem=yr_sem,
                    device_id=(0, d, t), device_id_type=MESH).start()
            return c

        with jax.named_scope("give"):
            lax.fori_loop(0, per, give, 0, unroll=True)
        return c

    lax.fori_loop(0, CHUNKS, finish, 0)

    @pl.when(here)
    def _():
        yrecv[dev] = ysend[(dev % 32) * 2 + side]

    def wait_blocks(ref, sem):
        @pl.when(here)
        def _():
            pltpu.make_async_copy(ref.at[pl.ds(0, 63)], ref.at[pl.ds(0, 63)], sem).wait()

        @pl.when(jnp.logical_not(here))
        def _():
            pltpu.make_async_copy(ref, ref, sem).wait()

    with jax.named_scope("yrwait"):
        wait_blocks(yrecv, yr_sem)
    with jax.named_scope("final"):
        x1 = jnp.concatenate([x1f[n] for n in range(6)], axis=1)
        x1 = jnp.where(side == 0, x1[0:4], x1[4:8])
        sums = []
        for j in range(GRP):
            acc = None
            for c in range(N_DEV):
                x, y, z = coords(c)
                if (x % 2) + 2 * (y % 2) + 4 * (z % 2) == j:
                    acc = yrecv[c] if acc is None else acc + yrecv[c]
            sums.append(acc)
        for j in range(GRP):
            y = jnp.where(dev // 32 == 0, sums[j], sums[GRP - 1 - j])
            out[:, j * NC:(j + 1) * NC] = (x1[:, j * NC:(j + 1) * NC] + y.astype(BF16).astype(F32)).astype(BF16)

    with jax.named_scope("drain"):
        for k in range(1, GRP):
            wd_copy(k).wait_send()
            for r in range(CHUNKS):
                u_copy(k, r).wait_send()
        for n in range(6):
            p_copy(n).wait_send()
        for q in range(3):
            some = wkv_b.at[0, pl.ds(0, 15 * 8)]
            pltpu.make_async_copy(some, some, a1s.at[q]).wait()
            most = hbuf.at[q, pl.ds(0, 3)]
            pltpu.make_async_copy(most, most, a2s.at[q]).wait()
        for r in range(CHUNKS):
            g_copy(r).wait_send()
        wait_blocks(ysend, ys_sem)


def solution(mesh):
    batch_axes = ('inst', 'dev')
    in_specs = (
        P(batch_axes, None),
        P(batch_axes),
        P(None, batch_axes, None, None, None),
        P(None, batch_axes, None, None, None),
        P(), P(), P(), P(), P(),
        P(None, None, 'dev'),
        P(None, None, 'dev'),
        P(None, 'dev', None),
    )
    out_specs = P(('inst', 'dev', 'side'), None)
    half = HEAD // 2
    freqs = (ROPE_BASE ** (-np.arange(half, dtype=np.float64) / half)).astype(np.float32)
    freqs = np.concatenate([freqs, freqs])[None]

    def device_fn(hidden, cache_len, k_cache, v_cache, w_q, w_kv, w_o, attn_gain, ffn_gain, w_gate, w_up, w_down):
        vmem = pl.BlockSpec(memory_space=pltpu.VMEM)
        hbm = pl.BlockSpec(memory_space=pl.ANY)
        dma = pltpu.SemaphoreType.DMA
        return pl.pallas_call(
            body,
            out_shape=jax.ShapeDtypeStruct((4, D), BF16),
            in_specs=[pl.BlockSpec(memory_space=pltpu.SMEM)] + [hbm] * 12,
            out_specs=vmem,
            scratch_shapes=[
                pltpu.VMEM((8, D), BF16),
                pltpu.VMEM((1, D), F32),
                pltpu.VMEM((6, 1, 512), F32),
                pltpu.VMEM((1, HEAD), F32),
                pltpu.VMEM((KVH, D, 384), BF16),
                pltpu.VMEM((2, D, 512), BF16),
                pltpu.VMEM((6, DH, 512), BF16),
                pltpu.VMEM((KVH, 8, SEQ, HEAD), BF16),
                pltpu.VMEM((KVH, 8, SEQ, HEAD), BF16),
                pltpu.VMEM((DH, 2 * FFC), BF16),
                pltpu.VMEM((GRP, FFC, NC), BF16),
                pltpu.VMEM((8, D), BF16),
                pltpu.VMEM((2, KVH, 8, HEAD), F32),
                pltpu.VMEM((KVH, 8, 384), BF16),
                pltpu.VMEM((6, 8, 512), F32),
                pltpu.VMEM((6, 8, 512), F32),
                pltpu.VMEM((6, 8, 512), F32),
                pltpu.VMEM((3, 4, 4, 4, 8, PART), BF16),
                pltpu.VMEM((2, CH, DH), BF16),
                pltpu.VMEM((CHUNKS, CH, 2 * FFC), F32),
                pltpu.VMEM((CHUNKS, CH, 2 * FFC), F32),
                pltpu.VMEM((CHUNKS, CH, 2 * FFC), F32),
                pltpu.VMEM((GRP, CHUNKS, CH, FFC), BF16),
                pltpu.VMEM((64, 4, NC), F32),
                pltpu.VMEM((64, 4, NC), F32),
                pltpu.VMEM((2, 8, 128), F32),
                pltpu.VMEM((24, 128), jnp.int32),
                dma((4,)), dma((KVH,)), dma((2, D // KVC)), dma((2, KVH)), dma((6,)), dma((2,)), dma, dma((GRP,)), dma((GRP,)),
                dma((6,)), dma((6,)), dma((3,)), dma((3, 4)), dma((3,)), dma((3, 2, 4)), dma((3, 4)), dma((CHUNKS,)), dma((CHUNKS,)),
                dma((GRP, CHUNKS)), dma((GRP, CHUNKS)), dma, dma,
            ],
            compiler_params=pltpu.CompilerParams(
                collective_id=0, has_side_effects=True, vmem_limit_bytes=60 * 1024 * 1024),
            name="decode_layer",
        )(cache_len, hidden, attn_gain, ffn_gain.reshape(6, 1, 512), jnp.asarray(freqs),
          k_cache, v_cache, w_q, w_kv, w_o, w_gate, w_up, w_down)

    return jax.shard_map(device_fn, mesh=mesh, in_specs=in_specs, out_specs=out_specs, check_vma=False)
```

```python
import numpy as np
import jax
import jax.numpy as jnp
from jax import lax
from jax.experimental import pallas as pl
from jax.experimental.pallas import tpu as pltpu
from jax.sharding import PartitionSpec as P

EPS = 1e-5
ROPE_BASE = 10000.0
MESH = pl.DeviceIdType.MESH
F32 = jnp.float32
BF16 = jnp.bfloat16

N_DEV = 64
D = 3072
DH = D // 2
PART = D // 3
FFC = 128
SEQ = 256
HEAD = 128
KVH = 4
GROUP = 3
GRP = 8
NC = D // GRP
ROWS = 256
CHUNKS = 4
CH = ROWS // CHUNKS
KVC = 768
ORDER = (0, 1, 3, 2)


def coords(dev):
    return dev % 4, (dev // 4) % 4, dev // 16


def flat(x, y, z):
    return z * 16 + y * 4 + x


def ring_slot(part, x, y, z):
    return ((x, z, y), (y, z, x), (z, y, x))[part]


def chip_at(part, ring, row, col):
    return (flat(ring, col, row), flat(col, ring, row), flat(col, row, ring))[part]


def body(lens, hid_h, again_h, fgain_h, freq_h, kc, vc, wq, wkv, wo, wg, wu, wd, out,
         hid, again, fgain, freq,
         wq_b, wkv_b, wo_b, kc_b, vc_b, wgu_b, wd_b, a_b, kv_b, o_b, p_own, p_oth, x1f,
         hbuf, h2, ubuf, ysend, yrecv, tab, lens_v,
         i_sem, w_sem, kv_sem, c_sem, wo_sem, f_sem, wd_sem, wds_sem, wdr_sem,
         ps_sem, pr_sem, a1s, a1r, a2s, a2r, a2f, us_sem, ur_sem, ys_sem, yr_sem):
    dev = lax.axis_index("dev")
    side = lax.axis_index("side")
    cx, cy, cz = coords(dev)
    j_me = (cx + side) % 2 + 2 * ((cy + side) % 2) + 4 * ((cz + side) % 2)

    source = (cx + cy + cz) % 2 == side

    def quadrant(r):
        dx, dy = ((1, 1), (1, 0), (0, 1), (0, 0))[r]
        qx = (((cx + side) % 4) // 2 + dx) % 2
        qy = (((cy + side) % 4) // 2 + dy) % 2
        return [(2 * qx + i + 4 - side) % 4 for i in range(2)], [(2 * qy + i + 4 - side) % 4 for i in range(2)]

    def height(x, y, i):
        return 2 * i + (side + x + y) % 2

    other = 1 - side

    def in_copy(i):
        src, dst = ((hid_h, hid), (again_h, again), (fgain_h, fgain), (freq_h, freq))[i]
        return pltpu.make_async_copy(src, dst, i_sem.at[i])

    def kv_copy(i, c):
        col = pl.multiple_of(i * 1024 + side * 512, 128)
        rows = pl.ds(c * KVC, KVC)
        return pltpu.make_async_copy(wkv.at[0, rows, pl.ds(col, 512)], wkv_b.at[i, rows], kv_sem.at[i, c])

    def q_copy(h):
        col = pl.multiple_of(side * DH + h * 384, 128)
        return pltpu.make_async_copy(wq.at[0, :, pl.ds(col, 384)], wq_b.at[h], w_sem.at[h])

    def c_copy(i, h):
        src, dst = (kc, kc_b) if i == 0 else (vc, vc_b)
        return pltpu.make_async_copy(src.at[0, :, side * KVH + h], dst.at[h], c_sem.at[i, h])

    def head_copies(h):
        q_copy(h).start()
        c_copy(0, h).start()
        c_copy(1, h).start()

    def o_copy(n):
        row = pl.multiple_of(side * DH, 128)
        return pltpu.make_async_copy(wo.at[0, pl.ds(row, DH), pl.ds(pl.multiple_of(n * 512, 128), 512)], wo_b.at[n], wo_sem.at[n])

    def f_copy(i):
        src = wg if i == 0 else wu
        return pltpu.make_async_copy(src.at[0], wgu_b.at[:, pl.ds(i * FFC, FFC)], f_sem.at[i])

    wd_own = pltpu.make_async_copy(wd.at[0, :, pl.ds(pl.multiple_of(j_me * NC, 128), NC)], wd_b.at[j_me], wd_sem)

    for i in range(4):
        in_copy(i).start()
    for c in range(D // KVC):
        kv_copy(0, c).start()

    barrier = pltpu.get_barrier_semaphore()

    def pair(c):
        return (c + 1 + 2 * ((c + side) % 2)) % 4

    def block_peer(k):
        px = pair(cx) if k % 2 else cx
        py = pair(cy) if (k // 2) % 2 else cy
        pz = pair(cz) if k // 4 else cz
        return flat(px, py, pz), (px + side) % 2 + 2 * ((py + side) % 2) + 4 * ((pz + side) % 2)

    def greet(d, t):
        pl.semaphore_signal(barrier, inc=1, device_id=(0, d, t), device_id_type=MESH)

    with jax.named_scope("greet"):
        greet(dev, other)
        greet(block_peer(GRP - 1)[0], side)
        for i in range(1, 64):
            ix, iy, iz = coords(i)
            if not (ix and iy and iz):
                greet(flat((cx + ix) % 4, (cy + iy) % 4, (cz + iz) % 4), side)
    greeted = 38

    with jax.named_scope("inwait"):
        for i in range(4):
            in_copy(i).wait()
    for c in range(D // KVC):
        kv_copy(1, c).start()

    with jax.named_scope("tables"):
        rowb = lax.broadcasted_iota(jnp.int32, (8, 128), 0)
        lv = jnp.zeros((8, 128), jnp.int32)
        for b in range(8):
            lv = jnp.where(rowb == b, lens[b], lv)
        angle = lv.astype(F32) * freq[...]
        lane = lax.broadcasted_iota(jnp.int32, (8, 128), 1)
        sin = jnp.sin(angle)
        tab[0] = jnp.cos(angle)
        tab[1] = jnp.where(lane < 64, -sin, sin)
        lens_v[...] = jnp.concatenate([lv, lv, lv], axis=0)

    def rotary(v):
        return v * tab[0] + pltpu.roll(v, 64, axis=1) * tab[1]

    with jax.named_scope("norm"):
        xf = hid[...].astype(F32)
        inv = lax.rsqrt(jnp.mean(xf * xf, axis=-1, keepdims=True) + EPS)
        a_b[...] = (xf * inv * again[...]).astype(BF16)

    for i in range(2):
        with jax.named_scope("kvwait"):
            for c in range(D // KVC):
                kv_copy(i, c).wait()
        head_copies(i)
        with jax.named_scope("kvdot"):
            kv = jnp.dot(a_b[...], wkv_b[i], preferred_element_type=F32)
            for h in range(KVH):
                v = kv[:, h * HEAD:(h + 1) * HEAD]
                if i == 0:
                    v = rotary(v)
                kv_b[i, h] = v.astype(BF16).astype(F32)

    rowm = lax.broadcasted_iota(jnp.int32, (24, SEQ), 0) % 8
    rowv = lax.broadcasted_iota(jnp.int32, (24, HEAD), 0) % 8
    pos = lax.broadcasted_iota(jnp.int32, (24, SEQ), 1)
    scale = HEAD ** -0.5

    def attend(h, c):
        with jax.named_scope("qwait"):
            q_copy(h).wait()

        @pl.when(h < 2)
        def _():
            head_copies(h + 2)

        @pl.when(h >= 2)
        def _():
            for i in range(3):
                o_copy(3 * (h - 2) + i).start()

        with jax.named_scope("qdot"):
            q = jnp.dot(a_b[...], wq_b[h], preferred_element_type=F32)
            qf = jnp.concatenate([rotary(q[:, g * HEAD:(g + 1) * HEAD]) for g in range(GROUP)], axis=0)
            qb = qf.astype(BF16)
        k_new = kv_b[0, h]
        v_new = kv_b[1, h]
        k3 = jnp.concatenate([k_new, k_new, k_new], axis=0)
        v3 = jnp.concatenate([v_new, v_new, v_new], axis=0)
        self_score = jnp.sum(qb.astype(F32) * k3, axis=-1, keepdims=True) * scale
        with jax.named_scope("cwait"):
            c_copy(0, h).wait()
            c_copy(1, h).wait()
        with jax.named_scope("mix"):
            s = jnp.zeros((24, SEQ), F32)
            for b in range(8):
                sb = lax.dot_general(qb, kc_b[h, b], (((1,), (1,)), ((), ())), preferred_element_type=F32)
                s = jnp.where(rowm == b, sb, s)
            limit = lens_v[...]
            limit = jnp.concatenate([limit, limit], axis=1)
            s = jnp.where(pos < limit, s * scale, -1e30)
            top = jnp.maximum(jnp.max(s, axis=-1, keepdims=True), self_score)
            e = jnp.exp(s - top)
            es = jnp.exp(self_score - top)
            total = jnp.sum(e, axis=-1, keepdims=True) + es
            eb = e.astype(BF16)
            m = jnp.zeros((24, HEAD), F32)
            for b in range(8):
                mb = jnp.dot(eb, vc_b[h, b], preferred_element_type=F32)
                m = jnp.where(rowv == b, mb, m)
            m = m + es.astype(BF16).astype(F32) * v3
            o = m / total
            for g in range(GROUP):
                o_b[h, :, g * HEAD:(g + 1) * HEAD] = o[g * 8:(g + 1) * 8].astype(BF16)
        return c

    lax.fori_loop(0, 2, attend, 0)
    with jax.named_scope("barrier"):
        pl.semaphore_wait(barrier, greeted)

    def wd_copy(k):
        peer, j = block_peer(k)
        return pltpu.make_async_remote_copy(
            src_ref=wd.at[0, :, pl.ds(pl.multiple_of(j * NC, 128), NC)], dst_ref=wd_b.at[j_me],
            send_sem=wds_sem.at[k], recv_sem=wdr_sem.at[k], device_id=(0, peer, side), device_id_type=MESH)

    with jax.named_scope("wdsend"):
        for k in range(1, GRP):
            wd_copy(k).start()

    lax.fori_loop(2, KVH, attend, 0)

    f_copy(0).start()
    f_copy(1).start()
    wd_own.start()

    def p_copy(n):
        return pltpu.make_async_remote_copy(
            src_ref=p_own.at[n], dst_ref=p_oth.at[n], send_sem=ps_sem.at[n], recv_sem=pr_sem.at[n],
            device_id=(0, dev, other), device_id_type=MESH)

    o_all = jnp.concatenate([o_b[h] for h in range(KVH)], axis=1)

    def project(n, c):
        o_copy(n).wait()
        p_own[n] = jnp.dot(o_all, wo_b[n], preferred_element_type=F32)
        p_copy(n).start()
        return c

    with jax.named_scope("project"):
        lax.fori_loop(0, 6, project, 0)

    with jax.named_scope("x1"):
        ssq = jnp.zeros((8, 1), F32)
        for n in range(6):
            p_copy(n).wait_recv()
            v = hid[:, n * 512:(n + 1) * 512].astype(F32) + (p_own[n] + p_oth[n])
            v = v.astype(BF16).astype(F32)
            x1f[n] = v
            ssq = ssq + jnp.sum(v * v, axis=-1, keepdims=True)
        inv1 = lax.rsqrt(ssq / D + EPS)

        at = [ring_slot(q, cx, cy, cz) for q in range(3)]

        @pl.when(source)
        def _():
            for n in range(6):
                ring, row, col = at[n // 2]
                v = x1f[n] * inv1 * fgain[n]
                hbuf[n // 2, ring, row, col // 2, :, (n % 2) * 512:(n % 2 + 1) * 512] = v.astype(BF16)

    with jax.named_scope("ag1send"):
        @pl.when(source)
        def _():
            for i in ORDER:
                for j in ORDER:
                    if i or j:
                        for q in range(3):
                            ring, row, col = at[q]
                            block = hbuf.at[q, ring, row, col // 2]
                            pltpu.make_async_remote_copy(
                                src_ref=block, dst_ref=block, send_sem=a1s.at[q], recv_sem=a1r.at[q, (4 - i) % 4],
                                device_id=(0, chip_at(q, ring, (row + i) % 4, (col + j) % 4), side),
                                device_id_type=MESH).start()

    def a2_copy(q, g, step, src, sem):
        ring, row, col = at[q]
        part = hbuf.at[q, src, (row + ORDER[g]) % 4]
        return pltpu.make_async_remote_copy(
            src_ref=part, dst_ref=part, send_sem=a2s.at[q], recv_sem=sem,
            device_id=(0, chip_at(q, (ring + step) % 4, row, col), side), device_id_type=MESH)

    def own_row(g):
        for q in range(3):
            if g == 0:
                @pl.when(source)
                def _(q=q):
                    some = hbuf.at[q, 0, 0, 0]
                    pltpu.make_async_copy(some, some, a1r.at[q, 0]).wait()

                @pl.when(jnp.logical_not(source))
                def _(q=q):
                    recv_row(q, a1r.at[q, 0])
            else:
                recv_row(q, a1r.at[q, ORDER[g]])
            ring = at[q][0]
            a2_copy(q, g, 1, ring, a2r.at[q, 0, g]).start()
            a2_copy(q, g, 3, ring, a2r.at[q, 1, g]).start()

    def recv_row(q, sem):
        some = hbuf.at[q, 0, 0]
        pltpu.make_async_copy(some, some, sem).wait()

    def pass_row(g):
        for q in range(3):
            ring = at[q][0]
            if g in (0, 3):
                recv_row(q, a2r.at[q, 0, g])
                a2_copy(q, g, 1, (ring + 3) % 4, a2f.at[q, g]).start()
            else:
                recv_row(q, a2r.at[q, 1, g])
                a2_copy(q, g, 3, (ring + 1) % 4, a2f.at[q, g]).start()

    for step, g in ((own_row, 0), (own_row, 1), (own_row, 2), (own_row, 3), (pass_row, 0), (pass_row, 1), (pass_row, 2), (pass_row, 3)):
        with jax.named_scope(f"{step.__name__}{g}"):
            step(g)
    with jax.named_scope("ag2wait"):
        for g in range(4):
            for q in range(3):
                recv_row(q, a2r.at[q, 1 if g in (0, 3) else 0, g])
        for g in range(4):
            for q in range(3):
                recv_row(q, a2f.at[q, g])

    f_copy(0).wait()
    f_copy(1).wait()

    def arrange(r):
        xs, ys = quadrant(r)
        for i in range(4):
            y, h = ys[i % 2], i // 2
            slots = [ring_slot_of(xs[t], y, height(xs[t], y, h)) for t in range(2)]
            for q in range(3):
                vs = [hbuf[q, ring, row, col // 2].astype(F32) for ring, row, col in (slot[q] for slot in slots)]
                h2[r % 2, i * 16:(i + 1) * 16, q * PART:(q + 1) * PART] = jnp.concatenate(vs, axis=0).astype(BF16)

    def ring_slot_of(x, y, z):
        return [ring_slot(q, x, y, z) for q in range(3)]

    def u_copy(k, r):
        peer, _ = block_peer(k)
        return pltpu.make_async_remote_copy(
            src_ref=ubuf.at[j_me, r], dst_ref=ubuf.at[j_me, r], send_sem=us_sem.at[k, r], recv_sem=ur_sem.at[k, r],
            device_id=(0, peer, side), device_id_type=MESH)

    for r in range(CHUNKS):
        with jax.named_scope("gateup"):
            arrange(r)
            both = jnp.dot(h2[r % 2], wgu_b[...], preferred_element_type=F32)
            gate = both[:, :FFC]
            up = both[:, FFC:]
            ubuf[j_me, r] = (gate * jax.nn.sigmoid(gate) * up).astype(BF16)
            for k in range(1, GRP):
                u_copy(k, r).start()

    wd_own.wait()
    with jax.named_scope("wdwait"):
        for k in range(1, GRP):
            wd_copy(k).wait_recv()

    per = 64 // CHUNKS

    fx, fy, fz = (cx + side) % 2, (cy + side) % 2, cz // 2

    def finish(r):
        with jax.named_scope("uwait"):
            for k in range(1, GRP):
                u_copy(k, r).wait_recv()
        with jax.named_scope("down"):
            u_all = jnp.concatenate([ubuf[j, r] for j in range(GRP)], axis=1)
            y = jnp.dot(u_all, wd_b[...].reshape(GRP * FFC, NC), preferred_element_type=F32)
            for i in range(per // 2):
                ysend[r * per + 2 * i] = y[i * 8:i * 8 + 4]
                ysend[r * per + 2 * i + 1] = y[i * 8 + 4:i * 8 + 8]
        with jax.named_scope("give"):
            xs, ys = quadrant(r)
            ax, ay, az = [(a + fx) % 2 for a in range(2)], [(a + fy) % 2 for a in range(2)], [(a + fz) % 2 for a in range(2)]
            px = [jnp.where(a == 0, xs[0], xs[1]) for a in ax]
            py = [jnp.where(a == 0, ys[0], ys[1]) for a in ay]
            for i in range(per):
                a, b, c, t = i % 2, (i // 2) % 2, 1 - (i // 4) % 2, i // 8
                k = 2 * (ax[a] + 2 * ay[b] + 4 * az[c]) + t
                d = flat(px[a], py[b], height(px[a], py[b], az[c]))

                def start(k=k, d=d, t=t):
                    pltpu.make_async_remote_copy(
                        src_ref=ysend.at[r * per + k], dst_ref=yrecv.at[dev], send_sem=ys_sem, recv_sem=yr_sem,
                        device_id=(0, d, t), device_id_type=MESH).start()

                if r == CHUNKS - 1 and not (a or b or c):
                    pl.when(jnp.logical_not(jnp.logical_and(source, side == t)))(start)
                else:
                    start()

    for r in range(CHUNKS):
        finish(r)

    @pl.when(source)
    def _():
        yrecv[dev] = ysend[(CHUNKS - 1) * per + 2 * (fx + 2 * fy + 4 * fz) + side]

    def wait_blocks(ref, sem):
        @pl.when(source)
        def _():
            pltpu.make_async_copy(ref.at[pl.ds(0, 63)], ref.at[pl.ds(0, 63)], sem).wait()

        @pl.when(jnp.logical_not(source))
        def _():
            pltpu.make_async_copy(ref, ref, sem).wait()

    with jax.named_scope("yrwait"):
        wait_blocks(yrecv, yr_sem)
    with jax.named_scope("final"):
        x1 = jnp.concatenate([x1f[n] for n in range(6)], axis=1)
        x1 = jnp.where(side == 0, x1[0:4], x1[4:8])
        sums = []
        for j in range(GRP):
            acc = None
            for c in range(N_DEV):
                x, y, z = coords(c)
                if (x % 2) + 2 * (y % 2) + 4 * (z % 2) == j:
                    acc = yrecv[c] if acc is None else acc + yrecv[c]
            sums.append(acc)
        for j in range(GRP):
            y = jnp.where((cx + cy + cz) % 2 == 0, sums[j], sums[GRP - 1 - j])
            out[:, j * NC:(j + 1) * NC] = (x1[:, j * NC:(j + 1) * NC] + y.astype(BF16).astype(F32)).astype(BF16)

    with jax.named_scope("drain"):
        for k in range(1, GRP):
            wd_copy(k).wait_send()
            for r in range(CHUNKS):
                u_copy(k, r).wait_send()
        for n in range(6):
            p_copy(n).wait_send()
        for q in range(3):
            @pl.when(source)
            def _(q=q):
                some = wkv_b.at[0, pl.ds(0, 15 * 16)]
                pltpu.make_async_copy(some, some, a1s.at[q]).wait()
            most = hbuf.at[q, pl.ds(0, 3)]
            pltpu.make_async_copy(most, most, a2s.at[q]).wait()
        wait_blocks(ysend, ys_sem)


def solution(mesh):
    batch_axes = ('inst', 'dev')
    in_specs = (
        P(batch_axes, None),
        P(batch_axes),
        P(None, batch_axes, None, None, None),
        P(None, batch_axes, None, None, None),
        P(), P(), P(), P(), P(),
        P(None, None, 'dev'),
        P(None, None, 'dev'),
        P(None, 'dev', None),
    )
    out_specs = P(('inst', 'dev', 'side'), None)
    half = HEAD // 2
    freqs = (ROPE_BASE ** (-np.arange(half, dtype=np.float64) / half)).astype(np.float32)
    freqs = np.concatenate([freqs, freqs])[None]

    def device_fn(hidden, cache_len, k_cache, v_cache, w_q, w_kv, w_o, attn_gain, ffn_gain, w_gate, w_up, w_down):
        vmem = pl.BlockSpec(memory_space=pltpu.VMEM)
        hbm = pl.BlockSpec(memory_space=pl.ANY)
        dma = pltpu.SemaphoreType.DMA
        return pl.pallas_call(
            body,
            out_shape=jax.ShapeDtypeStruct((4, D), BF16),
            in_specs=[pl.BlockSpec(memory_space=pltpu.SMEM)] + [hbm] * 12,
            out_specs=vmem,
            scratch_shapes=[
                pltpu.VMEM((8, D), BF16),
                pltpu.VMEM((1, D), F32),
                pltpu.VMEM((6, 1, 512), F32),
                pltpu.VMEM((1, HEAD), F32),
                pltpu.VMEM((KVH, D, 384), BF16),
                pltpu.VMEM((2, D, 512), BF16),
                pltpu.VMEM((6, DH, 512), BF16),
                pltpu.VMEM((KVH, 8, SEQ, HEAD), BF16),
                pltpu.VMEM((KVH, 8, SEQ, HEAD), BF16),
                pltpu.VMEM((D, 2 * FFC), BF16),
                pltpu.VMEM((GRP, FFC, NC), BF16),
                pltpu.VMEM((8, D), BF16),
                pltpu.VMEM((2, KVH, 8, HEAD), F32),
                pltpu.VMEM((KVH, 8, 384), BF16),
                pltpu.VMEM((6, 8, 512), F32),
                pltpu.VMEM((6, 8, 512), F32),
                pltpu.VMEM((6, 8, 512), F32),
                pltpu.VMEM((3, 4, 4, 2, 8, PART), BF16),
                pltpu.VMEM((2, CH, D), BF16),
                pltpu.VMEM((GRP, CHUNKS, CH, FFC), BF16),
                pltpu.VMEM((64, 4, NC), F32),
                pltpu.VMEM((64, 4, NC), F32),
                pltpu.VMEM((2, 8, 128), F32),
                pltpu.VMEM((24, 128), jnp.int32),
                dma((4,)), dma((KVH,)), dma((2, D // KVC)), dma((2, KVH)), dma((6,)), dma((2,)), dma, dma((GRP,)), dma((GRP,)),
                dma((6,)), dma((6,)), dma((3,)), dma((3, 4)), dma((3,)), dma((3, 2, 4)), dma((3, 4)),
                dma((GRP, CHUNKS)), dma((GRP, CHUNKS)), dma, dma,
            ],
            compiler_params=pltpu.CompilerParams(
                collective_id=0, has_side_effects=True, vmem_limit_bytes=60 * 1024 * 1024),
            name="decode_layer",
        )(cache_len, hidden, attn_gain, ffn_gain.reshape(6, 1, 512), jnp.asarray(freqs),
          k_cache, v_cache, w_q, w_kv, w_o, w_gate, w_up, w_down)

    return jax.shard_map(device_fn, mesh=mesh, in_specs=in_specs, out_specs=out_specs, check_vma=False)
```

```python
import numpy as np
import jax
import jax.numpy as jnp
from jax import lax
from jax.experimental import pallas as pl
from jax.experimental.pallas import tpu as pltpu
from jax.sharding import PartitionSpec as P

EPS = 1e-5
ROPE_BASE = 10000.0
MESH = pl.DeviceIdType.MESH
F32 = jnp.float32
BF16 = jnp.bfloat16

N_DEV = 64
D = 3072
DH = D // 2
PART = D // 3
FFC = 128
SEQ = 256
HEAD = 128
KVH = 4
GROUP = 3
GRP = 8
NC = D // GRP
ROWS = 256
CHUNKS = 2
CH = ROWS // CHUNKS
KVC = 768
ORDER = (0, 1, 3, 2)


def coords(dev):
    return dev % 4, (dev // 4) % 4, dev // 16


def flat(x, y, z):
    return z * 16 + y * 4 + x


def ring_slot(part, x, y, z):
    return ((x, z, y), (y, z, x), (z, y, x))[part]


def chip_at(part, ring, row, col):
    return (flat(ring, col, row), flat(col, ring, row), flat(col, row, ring))[part]


def body(lens, hid_h, again_h, fgain_h, freq_h, kc, vc, wq, wkv, wo, wg, wu, wd, out,
         hid, again, fgain, freq,
         wq_b, wkv_b, wo_b, kc_b, vc_b, wgu_b, wd_b, a_b, kv_b, o_b, p_own, p_oth, x1f,
         hbuf, h2, ubuf, ysend, yrecv, tab, lens_v,
         i_sem, w_sem, kv_sem, c_sem, wo_sem, f_sem, wd_sem, wds_sem, wdr_sem,
         ps_sem, pr_sem, a1s, a1r, a2s, a2r, us_sem, ur_sem, ys_sem, yr_sem):
    dev = lax.axis_index("dev")
    side = lax.axis_index("side")
    cx, cy, cz = coords(dev)
    j_me = (cx + side) % 2 + 2 * ((cy + side) % 2) + 4 * ((cz + side) % 2)

    source = (cx + cy + cz) % 2 == side

    def half(r):
        qx = (((cx + side) % 4) // 2 + 1 - r) % 2
        return [(2 * qx + i + 4 - side) % 4 for i in range(2)]

    def height(x, y, i):
        return 2 * i + (side + x + y) % 2

    other = 1 - side

    def in_copy(i):
        src, dst = ((hid_h, hid), (again_h, again), (fgain_h, fgain), (freq_h, freq))[i]
        return pltpu.make_async_copy(src, dst, i_sem.at[i])

    def kv_copy(i, c):
        col = pl.multiple_of(i * 1024 + side * 512, 128)
        rows = pl.ds(c * KVC, KVC)
        return pltpu.make_async_copy(wkv.at[0, rows, pl.ds(col, 512)], wkv_b.at[i, rows], kv_sem.at[i, c])

    def q_copy(h):
        col = pl.multiple_of(side * DH + h * 768, 128)
        return pltpu.make_async_copy(wq.at[0, :, pl.ds(col, 768)], wq_b.at[h], w_sem.at[h])

    def c_copy(i, h):
        src, dst = (kc, kc_b) if i == 0 else (vc, vc_b)
        return pltpu.make_async_copy(src.at[0, :, pl.ds(side * KVH + 2 * h, 2)], dst.at[h], c_sem.at[i, h])

    def head_copies(h):
        q_copy(h).start()
        c_copy(0, h).start()
        c_copy(1, h).start()

    def o_copy(n):
        row = pl.multiple_of(side * DH, 128)
        return pltpu.make_async_copy(wo.at[0, pl.ds(row, DH), pl.ds(pl.multiple_of(n * 512, 128), 512)], wo_b.at[n], wo_sem.at[n])

    def f_copy(i):
        src = wg if i == 0 else wu
        return pltpu.make_async_copy(src.at[0], wgu_b.at[:, pl.ds(i * FFC, FFC)], f_sem.at[i])

    wd_own = pltpu.make_async_copy(wd.at[0, :, pl.ds(pl.multiple_of(j_me * NC, 128), NC)], wd_b.at[j_me], wd_sem)

    for i in range(4):
        in_copy(i).start()
    for c in range(D // KVC):
        kv_copy(0, c).start()

    barrier = pltpu.get_barrier_semaphore()

    def pair(c):
        return (c + 1 + 2 * ((c + side) % 2)) % 4

    def block_peer(k):
        px = pair(cx) if k % 2 else cx
        py = pair(cy) if (k // 2) % 2 else cy
        pz = pair(cz) if k // 4 else cz
        return flat(px, py, pz), (px + side) % 2 + 2 * ((py + side) % 2) + 4 * ((pz + side) % 2)

    def greet(d, t):
        pl.semaphore_signal(barrier, inc=1, device_id=(0, d, t), device_id_type=MESH)

    with jax.named_scope("greet"):
        greet(dev, other)
        greet(block_peer(GRP - 1)[0], side)
        for i in range(1, 64):
            ix, iy, iz = coords(i)
            if not (ix and iy and iz):
                greet(flat((cx + ix) % 4, (cy + iy) % 4, (cz + iz) % 4), side)
    greeted = 38

    for c in range(D // KVC):
        kv_copy(1, c).start()

    with jax.named_scope("inwait"):
        for i in range(4):
            in_copy(i).wait()

    with jax.named_scope("tables"):
        rowb = lax.broadcasted_iota(jnp.int32, (8, 128), 0)
        lv = jnp.zeros((8, 128), jnp.int32)
        for b in range(8):
            lv = jnp.where(rowb == b, lens[b], lv)
        angle = lv.astype(F32) * freq[...]
        lane = lax.broadcasted_iota(jnp.int32, (8, 128), 1)
        sin = jnp.sin(angle)
        tab[0] = jnp.cos(angle)
        tab[1] = jnp.where(lane < 64, -sin, sin)
        lens_v[...] = jnp.concatenate([lv, lv, lv], axis=0)

    def rotary(v):
        return v * tab[0] + pltpu.roll(v, 64, axis=1) * tab[1]

    with jax.named_scope("norm"):
        xf = hid[...].astype(F32)
        inv = lax.rsqrt(jnp.mean(xf * xf, axis=-1, keepdims=True) + EPS)
        a_b[...] = (xf * inv * again[...]).astype(BF16)

    for i in range(2):
        with jax.named_scope("kvwait"):
            for c in range(D // KVC):
                kv_copy(i, c).wait()
        head_copies(i)
        with jax.named_scope("kvdot"):
            kv = jnp.dot(a_b[...], wkv_b[i], preferred_element_type=F32)
            for h in range(KVH):
                v = kv[:, h * HEAD:(h + 1) * HEAD]
                if i == 0:
                    v = rotary(v)
                kv_b[i, h] = v.astype(BF16).astype(F32)

    rowm = lax.broadcasted_iota(jnp.int32, (24, SEQ), 0) % 8
    rowv = lax.broadcasted_iota(jnp.int32, (24, HEAD), 0) % 8
    pos = lax.broadcasted_iota(jnp.int32, (24, SEQ), 1)
    scale = HEAD ** -0.5

    def attend(p):
        with jax.named_scope("qwait"):
            q_copy(p).wait()
        for i in range(3):
            o_copy(3 * p + i).start()
        with jax.named_scope("qdot"):
            q = jnp.dot(a_b[...], wq_b[p], preferred_element_type=F32)
            qbs = [jnp.concatenate([rotary(q[:, (h * GROUP + g) * HEAD:(h * GROUP + g + 1) * HEAD]) for g in range(GROUP)], axis=0).astype(BF16)
                   for h in range(2)]
        with jax.named_scope("cwait"):
            c_copy(0, p).wait()
            c_copy(1, p).wait()
        with jax.named_scope("mix"):
            limit = lens_v[...]
            limit = jnp.concatenate([limit, limit], axis=1)
            scores = []
            for h in range(2):
                s = jnp.zeros((24, SEQ), F32)
                for b in range(8):
                    sb = lax.dot_general(qbs[h], kc_b[p, b, h], (((1,), (1,)), ((), ())), preferred_element_type=F32)
                    s = jnp.where(rowm == b, sb, s)
                scores.append(jnp.where(pos < limit, s * scale, -1e30))
            mixed = []
            for h in range(2):
                s = scores[h]
                k_new = kv_b[0, 2 * p + h]
                k3 = jnp.concatenate([k_new, k_new, k_new], axis=0)
                self_score = jnp.sum(qbs[h].astype(F32) * k3, axis=-1, keepdims=True) * scale
                top = jnp.maximum(jnp.max(s, axis=-1, keepdims=True), self_score)
                e = jnp.exp(s - top)
                es = jnp.exp(self_score - top)
                total = jnp.sum(e, axis=-1, keepdims=True) + es
                mixed.append((e.astype(BF16), es, total))
            for h in range(2):
                eb, es, total = mixed[h]
                m = jnp.zeros((24, HEAD), F32)
                for b in range(8):
                    mb = jnp.dot(eb, vc_b[p, b, h], preferred_element_type=F32)
                    m = jnp.where(rowv == b, mb, m)
                v_new = kv_b[1, 2 * p + h]
                v3 = jnp.concatenate([v_new, v_new, v_new], axis=0)
                m = m + es.astype(BF16).astype(F32) * v3
                o = m / total
                for g in range(GROUP):
                    o_b[2 * p + h, :, g * HEAD:(g + 1) * HEAD] = o[g * 8:(g + 1) * 8].astype(BF16)

    attend(0)
    with jax.named_scope("barrier"):
        pl.semaphore_wait(barrier, greeted)

    def wd_copy(k):
        peer, j = block_peer(k)
        return pltpu.make_async_remote_copy(
            src_ref=wd.at[0, :, pl.ds(pl.multiple_of(j * NC, 128), NC)], dst_ref=wd_b.at[j_me],
            send_sem=wds_sem.at[k], recv_sem=wdr_sem.at[k], device_id=(0, peer, side), device_id_type=MESH)

    with jax.named_scope("wdsend"):
        for k in range(1, GRP):
            wd_copy(k).start()

    attend(1)

    f_copy(0).start()
    f_copy(1).start()
    wd_own.start()

    def p_copy(n):
        return pltpu.make_async_remote_copy(
            src_ref=p_own.at[n], dst_ref=p_oth.at[n], send_sem=ps_sem.at[n], recv_sem=pr_sem.at[n],
            device_id=(0, dev, other), device_id_type=MESH)

    o_all = jnp.concatenate([o_b[h] for h in range(KVH)], axis=1)

    def project(n, c):
        o_copy(n).wait()
        p_own[n] = jnp.dot(o_all, wo_b[n], preferred_element_type=F32)
        p_copy(n).start()
        return c

    with jax.named_scope("project"):
        lax.fori_loop(0, 6, project, 0)

    with jax.named_scope("x1"):
        ssq = jnp.zeros((8, 1), F32)
        for n in range(6):
            p_copy(n).wait_recv()
            v = hid[:, n * 512:(n + 1) * 512].astype(F32) + (p_own[n] + p_oth[n])
            v = v.astype(BF16).astype(F32)
            x1f[n] = v
            ssq = ssq + jnp.sum(v * v, axis=-1, keepdims=True)
        inv1 = lax.rsqrt(ssq / D + EPS)

        at = [ring_slot(q, cx, cy, cz) for q in range(3)]

        @pl.when(source)
        def _():
            for n in range(6):
                ring, row, col = at[n // 2]
                v = x1f[n] * inv1 * fgain[n]
                hbuf[n // 2, ring, row, col // 2, :, (n % 2) * 512:(n % 2 + 1) * 512] = v.astype(BF16)

    with jax.named_scope("ag1send"):
        @pl.when(source)
        def _():
            for i in ORDER:
                for j in ORDER:
                    if i or j:
                        for q in range(3):
                            ring, row, col = at[q]
                            block = hbuf.at[q, ring, row, col // 2]
                            pltpu.make_async_remote_copy(
                                src_ref=block, dst_ref=block, send_sem=a1s.at[q], recv_sem=a1r.at[q, (4 - i) % 4],
                                device_id=(0, chip_at(q, ring, (row + i) % 4, (col + j) % 4), side),
                                device_id_type=MESH).start()

    def recv_row(q, sem):
        some = hbuf.at[q, 0, 0]
        pltpu.make_async_copy(some, some, sem).wait()

    def own_row(g, q):
        if g == 0:
            @pl.when(source)
            def _():
                some = hbuf.at[q, 0, 0, 0]
                pltpu.make_async_copy(some, some, a1r.at[q, 0]).wait()

            @pl.when(jnp.logical_not(source))
            def _():
                recv_row(q, a1r.at[q, 0])
        else:
            recv_row(q, a1r.at[q, ORDER[g]])
        ring, row, col = at[q]
        part = hbuf.at[q, ring, (row + ORDER[g]) % 4]
        for step in (2, 1, 3):
            pltpu.make_async_remote_copy(
                src_ref=part, dst_ref=part, send_sem=a2s.at[q], recv_sem=a2r.at[q],
                device_id=(0, chip_at(q, (ring + step) % 4, row, col), side), device_id_type=MESH).start()

    for g in range(4):
        with jax.named_scope(f"own_row{g}"):
            for q in range(3):
                own_row(g, q)
    with jax.named_scope("ag2wait"):
        for q in range(3):
            most = hbuf.at[q, pl.ds(0, 3)]
            pltpu.make_async_copy(most, most, a2r.at[q]).wait()

    f_copy(0).wait()
    f_copy(1).wait()

    def arrange(r):
        xs = half(r)
        for i in range(8):
            y, h = i % 4, i // 4
            zs = [height(x, y, h) for x in xs]
            slots = [((xs[t], zs[t], y // 2), (y, zs[t], xs[t] // 2), (zs[t], y, xs[t] // 2)) for t in range(2)]
            for q in range(3):
                vs = [hbuf[q, ring, row, col].astype(F32) for ring, row, col in (slot[q] for slot in slots)]
                h2[r % 2, i * 16:(i + 1) * 16, q * PART:(q + 1) * PART] = jnp.concatenate(vs, axis=0).astype(BF16)

    def u_copy(k, r):
        peer, _ = block_peer(k)
        return pltpu.make_async_remote_copy(
            src_ref=ubuf.at[j_me, r], dst_ref=ubuf.at[j_me, r], send_sem=us_sem.at[k, r], recv_sem=ur_sem.at[k, r],
            device_id=(0, peer, side), device_id_type=MESH)

    for r in range(CHUNKS):
        with jax.named_scope("gateup"):
            arrange(r)
            both = jnp.dot(h2[r % 2], wgu_b[...], preferred_element_type=F32)
            gate = both[:, :FFC]
            up = both[:, FFC:]
            ubuf[j_me, r] = (gate * jax.nn.sigmoid(gate) * up).astype(BF16)
            for k in range(1, GRP):
                u_copy(k, r).start()

    wd_own.wait()
    with jax.named_scope("wdwait"):
        for k in range(1, GRP):
            wd_copy(k).wait_recv()

    per = 64 // CHUNKS

    fx, fz = (cx + side) % 2, cz // 2

    def finish(r):
        with jax.named_scope("uwait"):
            for k in range(1, GRP):
                u_copy(k, r).wait_recv()
        with jax.named_scope("down"):
            u_all = jnp.concatenate([ubuf[j, r] for j in range(GRP)], axis=1)
            y = jnp.dot(u_all, wd_b[...].reshape(GRP * FFC, NC), preferred_element_type=F32)
            for i in range(per // 2):
                ysend[r * per + 2 * i] = y[i * 8:i * 8 + 4]
                ysend[r * per + 2 * i + 1] = y[i * 8 + 4:i * 8 + 8]
        with jax.named_scope("give"):
            xs = half(r)
            ax, ay, az = [(a + fx) % 2 for a in range(2)], [(b + cy) % 4 for b in range(4)], [(c + fz) % 2 for c in range(2)]
            px = [jnp.where(a == 0, xs[0], xs[1]) for a in ax]
            for i in range(per):
                a, b, c, t = i % 2, 3 - (i // 2) % 4, 1 - (i // 8) % 2, i // 16
                k = 2 * (ax[a] + 2 * ay[b] + 8 * az[c]) + t
                d = flat(px[a], ay[b], height(px[a], ay[b], az[c]))

                def start(k=k, d=d, t=t):
                    pltpu.make_async_remote_copy(
                        src_ref=ysend.at[r * per + k], dst_ref=yrecv.at[dev], send_sem=ys_sem, recv_sem=yr_sem,
                        device_id=(0, d, t), device_id_type=MESH).start()

                if r == CHUNKS - 1 and not (a or b or c):
                    pl.when(jnp.logical_not(jnp.logical_and(source, side == t)))(start)
                else:
                    start()

    for r in range(CHUNKS):
        finish(r)

    @pl.when(source)
    def _():
        yrecv[dev] = ysend[(CHUNKS - 1) * per + 2 * (fx + 2 * cy + 8 * fz) + side]

    def wait_blocks(ref, sem):
        @pl.when(source)
        def _():
            pltpu.make_async_copy(ref.at[pl.ds(0, 63)], ref.at[pl.ds(0, 63)], sem).wait()

        @pl.when(jnp.logical_not(source))
        def _():
            pltpu.make_async_copy(ref, ref, sem).wait()

    with jax.named_scope("yrwait"):
        wait_blocks(yrecv, yr_sem)
    with jax.named_scope("final"):
        x1 = jnp.concatenate([x1f[n] for n in range(6)], axis=1)
        x1 = jnp.where(side == 0, x1[0:4], x1[4:8])
        sums = []
        for j in range(GRP):
            acc = None
            for c in range(N_DEV):
                x, y, z = coords(c)
                if (x % 2) + 2 * (y % 2) + 4 * (z % 2) == j:
                    acc = yrecv[c] if acc is None else acc + yrecv[c]
            sums.append(acc)
        for j in range(GRP):
            y = jnp.where((cx + cy + cz) % 2 == 0, sums[j], sums[GRP - 1 - j])
            out[:, j * NC:(j + 1) * NC] = (x1[:, j * NC:(j + 1) * NC] + y.astype(BF16).astype(F32)).astype(BF16)

    with jax.named_scope("drain"):
        for k in range(1, GRP):
            wd_copy(k).wait_send()
            for r in range(CHUNKS):
                u_copy(k, r).wait_send()
        for n in range(6):
            p_copy(n).wait_send()
        for q in range(3):
            @pl.when(source)
            def _(q=q):
                some = wkv_b.at[0, pl.ds(0, 15 * 16)]
                pltpu.make_async_copy(some, some, a1s.at[q]).wait()
            most = hbuf.at[q, pl.ds(0, 3)]
            pltpu.make_async_copy(most, most, a2s.at[q]).wait()
        wait_blocks(ysend, ys_sem)


def solution(mesh):
    batch_axes = ('inst', 'dev')
    in_specs = (
        P(batch_axes, None),
        P(batch_axes),
        P(None, batch_axes, None, None, None),
        P(None, batch_axes, None, None, None),
        P(), P(), P(), P(), P(),
        P(None, None, 'dev'),
        P(None, None, 'dev'),
        P(None, 'dev', None),
    )
    out_specs = P(('inst', 'dev', 'side'), None)
    half = HEAD // 2
    freqs = (ROPE_BASE ** (-np.arange(half, dtype=np.float64) / half)).astype(np.float32)
    freqs = np.concatenate([freqs, freqs])[None]

    def device_fn(hidden, cache_len, k_cache, v_cache, w_q, w_kv, w_o, attn_gain, ffn_gain, w_gate, w_up, w_down):
        vmem = pl.BlockSpec(memory_space=pltpu.VMEM)
        hbm = pl.BlockSpec(memory_space=pl.ANY)
        dma = pltpu.SemaphoreType.DMA
        return pl.pallas_call(
            body,
            out_shape=jax.ShapeDtypeStruct((4, D), BF16),
            in_specs=[pl.BlockSpec(memory_space=pltpu.SMEM)] + [hbm] * 12,
            out_specs=vmem,
            scratch_shapes=[
                pltpu.VMEM((8, D), BF16),
                pltpu.VMEM((1, D), F32),
                pltpu.VMEM((6, 1, 512), F32),
                pltpu.VMEM((1, HEAD), F32),
                pltpu.VMEM((2, D, 768), BF16),
                pltpu.VMEM((2, D, 512), BF16),
                pltpu.VMEM((6, DH, 512), BF16),
                pltpu.VMEM((2, 8, 2, SEQ, HEAD), BF16),
                pltpu.VMEM((2, 8, 2, SEQ, HEAD), BF16),
                pltpu.VMEM((D, 2 * FFC), BF16),
                pltpu.VMEM((GRP, FFC, NC), BF16),
                pltpu.VMEM((8, D), BF16),
                pltpu.VMEM((2, KVH, 8, HEAD), F32),
                pltpu.VMEM((KVH, 8, 384), BF16),
                pltpu.VMEM((6, 8, 512), F32),
                pltpu.VMEM((6, 8, 512), F32),
                pltpu.VMEM((6, 8, 512), F32),
                pltpu.VMEM((3, 4, 4, 2, 8, PART), BF16),
                pltpu.VMEM((2, CH, D), BF16),
                pltpu.VMEM((GRP, CHUNKS, CH, FFC), BF16),
                pltpu.VMEM((64, 4, NC), F32),
                pltpu.VMEM((64, 4, NC), F32),
                pltpu.VMEM((2, 8, 128), F32),
                pltpu.VMEM((24, 128), jnp.int32),
                dma((4,)), dma((2,)), dma((2, D // KVC)), dma((2, 2)), dma((6,)), dma((2,)), dma, dma((GRP,)), dma((GRP,)),
                dma((6,)), dma((6,)), dma((3,)), dma((3, 4)), dma((3,)), dma((3,)),
                dma((GRP, CHUNKS)), dma((GRP, CHUNKS)), dma, dma,
            ],
            compiler_params=pltpu.CompilerParams(
                collective_id=0, has_side_effects=True, vmem_limit_bytes=60 * 1024 * 1024),
            name="decode_layer",
        )(cache_len, hidden, attn_gain, ffn_gain.reshape(6, 1, 512), jnp.asarray(freqs),
          k_cache, v_cache, w_q, w_kv, w_o, w_gate, w_up, w_down)

    return jax.shard_map(device_fn, mesh=mesh, in_specs=in_specs, out_specs=out_specs, check_vma=False)
```

```python
import numpy as np
import jax
import jax.numpy as jnp
from jax import lax
from jax.experimental import pallas as pl
from jax.experimental.pallas import tpu as pltpu
from jax.sharding import PartitionSpec as P

EPS = 1e-5
ROPE_BASE = 10000.0
MESH = pl.DeviceIdType.MESH
F32 = jnp.float32
BF16 = jnp.bfloat16

N_DEV = 64
D = 3072
DH = D // 2
PART = D // 3
FFC = 128
SEQ = 256
HEAD = 128
KVH = 4
GROUP = 3
GRP = 8
NC = D // GRP
ROWS = 256
CHUNKS = 2
CH = ROWS // CHUNKS
KVC = 768
ORDER = (0, 1, 3, 2)


def coords(dev):
    return dev % 4, (dev // 4) % 4, dev // 16


def flat(x, y, z):
    return z * 16 + y * 4 + x


def ring_slot(part, x, y, z):
    return ((x, z, y), (y, z, x), (z, y, x))[part]


def chip_at(part, ring, row, col):
    return (flat(ring, col, row), flat(col, ring, row), flat(col, row, ring))[part]


def body(lens_h, hid_h, again_h, fgain_h, freq_h, kc, vc, wq, wkv, wo, wg, wu, wd, out,
         lens, hid, again, fgain, freq,
         wq_b, wkv_b, wo_b, kc_b, vc_b, wgu_b, wd_b, a_b, kv_b, o_b, p_own, p_oth, x1f,
         hbuf, h2, ubuf, ysend, yrecv, tab, lens_v,
         i_sem, w_sem, kv_sem, c_sem, wo_sem, f_sem, wd_sem, wds_sem, wdr_sem,
         ps_sem, pr_sem, a1s, a1r, a2s, a2r, us_sem, ur_sem, ys_sem, yr_sem):
    dev = lax.axis_index("dev")
    side = lax.axis_index("side")
    cx, cy, cz = coords(dev)
    j_me = (cx + side) % 2 + 2 * ((cy + side) % 2) + 4 * ((cz + side) % 2)

    source = (cx + cy + cz) % 2 == side

    def half(r):
        qx = (((cx + side) % 4) // 2 + 1 - r) % 2
        return [(2 * qx + i + 4 - side) % 4 for i in range(2)]

    def height(x, y, i):
        return 2 * i + (side + x + y) % 2

    other = 1 - side

    def in_copy(i):
        src, dst = ((hid_h, hid), (again_h, again), (fgain_h, fgain), (freq_h, freq), (lens_h, lens))[i]
        return pltpu.make_async_copy(src, dst, i_sem.at[i])

    def kv_copy(i, c):
        col = pl.multiple_of(i * 1024 + side * 512, 128)
        rows = pl.ds(c * KVC, KVC)
        return pltpu.make_async_copy(wkv.at[0, rows, pl.ds(col, 512)], wkv_b.at[i, rows], kv_sem.at[i])

    def q_copy(h):
        col = pl.multiple_of(side * DH + h * 768, 128)
        return pltpu.make_async_copy(wq.at[0, :, pl.ds(col, 768)], wq_b.at[h], w_sem.at[h])

    def c_copy(i, h):
        src, dst = (kc, kc_b) if i == 0 else (vc, vc_b)
        return pltpu.make_async_copy(src.at[0, :, pl.ds(side * KVH + 2 * h, 2)], dst.at[h], c_sem.at[i, h])

    def head_copies(h):
        q_copy(h).start()
        c_copy(0, h).start()
        c_copy(1, h).start()

    def o_copy(n):
        row = pl.multiple_of(side * DH, 128)
        return pltpu.make_async_copy(wo.at[0, pl.ds(row, DH), pl.ds(pl.multiple_of(n * 512, 128), 512)], wo_b.at[n], wo_sem.at[n])

    def f_copy(i):
        src = wg if i == 0 else wu
        return pltpu.make_async_copy(src.at[0], wgu_b.at[:, pl.ds(i * FFC, FFC)], f_sem.at[i])

    wd_own = pltpu.make_async_copy(wd.at[0, :, pl.ds(pl.multiple_of(j_me * NC, 128), NC)], wd_b.at[j_me], wd_sem)

    for i in range(5):
        in_copy(i).start()
    for c in range(D // KVC):
        kv_copy(0, c).start()

    barrier = pltpu.get_barrier_semaphore()

    def pair(c):
        return (c + 1 + 2 * ((c + side) % 2)) % 4

    def block_peer(k):
        px = pair(cx) if k % 2 else cx
        py = pair(cy) if (k // 2) % 2 else cy
        pz = pair(cz) if k // 4 else cz
        return flat(px, py, pz), (px + side) % 2 + 2 * ((py + side) % 2) + 4 * ((pz + side) % 2)

    def greet(d, t):
        pl.semaphore_signal(barrier, inc=1, device_id=(0, d, t), device_id_type=MESH)

    with jax.named_scope("greet"):
        greet(dev, other)
        greet(block_peer(GRP - 1)[0], side)
        for i in range(1, 64):
            ix, iy, iz = coords(i)
            if not (ix and iy and iz):
                greet(flat((cx + ix) % 4, (cy + iy) % 4, (cz + iz) % 4), side)
    greeted = 38

    for c in range(D // KVC):
        kv_copy(1, c).start()

    with jax.named_scope("inwait"):
        for i in range(5):
            in_copy(i).wait()

    with jax.named_scope("tables"):
        rowb = lax.broadcasted_iota(jnp.int32, (8, 128), 0)
        lv = jnp.zeros((8, 128), jnp.int32)
        for b in range(8):
            lv = jnp.where(rowb == b, lens[b], lv)
        angle = lv.astype(F32) * freq[...]
        lane = lax.broadcasted_iota(jnp.int32, (8, 128), 1)
        sin = jnp.sin(angle)
        tab[0] = jnp.cos(angle)
        tab[1] = jnp.where(lane < 64, -sin, sin)
        lens_v[...] = jnp.concatenate([lv, lv, lv], axis=0)

    def rotary(v):
        return v * tab[0] + pltpu.roll(v, 64, axis=1) * tab[1]

    with jax.named_scope("norm"):
        xf = hid[...].astype(F32)
        inv = lax.rsqrt(jnp.mean(xf * xf, axis=-1, keepdims=True) + EPS)
        a_b[...] = (xf * inv * again[...]).astype(BF16)

    for i in range(2):
        with jax.named_scope("kvwait"):
            pltpu.make_async_copy(wkv_b.at[i], wkv_b.at[i], kv_sem.at[i]).wait()
        head_copies(i)
        with jax.named_scope("kvdot"):
            kv = jnp.dot(a_b[...], wkv_b[i], preferred_element_type=F32)
            for h in range(KVH):
                v = kv[:, h * HEAD:(h + 1) * HEAD]
                if i == 0:
                    v = rotary(v)
                kv_b[i, h] = v.astype(BF16).astype(F32)

    rowm = lax.broadcasted_iota(jnp.int32, (24, SEQ), 0) % 8
    rowv = lax.broadcasted_iota(jnp.int32, (24, HEAD), 0) % 8
    pos = lax.broadcasted_iota(jnp.int32, (24, SEQ), 1)
    scale = HEAD ** -0.5

    def attend(p):
        with jax.named_scope("qwait"):
            q_copy(p).wait()
        for i in range(3):
            o_copy(3 * p + i).start()
        with jax.named_scope("qdot"):
            q = jnp.dot(a_b[...], wq_b[p], preferred_element_type=F32)
            qbs = [jnp.concatenate([rotary(q[:, (h * GROUP + g) * HEAD:(h * GROUP + g + 1) * HEAD]) for g in range(GROUP)], axis=0).astype(BF16)
                   for h in range(2)]
        with jax.named_scope("cwait"):
            c_copy(0, p).wait()
            c_copy(1, p).wait()
        with jax.named_scope("mix"):
            limit = lens_v[...]
            limit = jnp.concatenate([limit, limit], axis=1)
            scores = []
            for h in range(2):
                s = jnp.zeros((24, SEQ), F32)
                for b in range(8):
                    sb = lax.dot_general(qbs[h], kc_b[p, b, h], (((1,), (1,)), ((), ())), preferred_element_type=F32)
                    s = jnp.where(rowm == b, sb, s)
                scores.append(jnp.where(pos < limit, s * scale, -1e30))
            mixed = []
            for h in range(2):
                s = scores[h]
                k_new = kv_b[0, 2 * p + h]
                k3 = jnp.concatenate([k_new, k_new, k_new], axis=0)
                self_score = jnp.sum(qbs[h].astype(F32) * k3, axis=-1, keepdims=True) * scale
                top = jnp.maximum(jnp.max(s, axis=-1, keepdims=True), self_score)
                e = jnp.exp(s - top)
                es = jnp.exp(self_score - top)
                total = jnp.sum(e, axis=-1, keepdims=True) + es
                mixed.append((e.astype(BF16), es, total))
            for h in range(2):
                eb, es, total = mixed[h]
                m = jnp.zeros((24, HEAD), F32)
                for b in range(8):
                    mb = jnp.dot(eb, vc_b[p, b, h], preferred_element_type=F32)
                    m = jnp.where(rowv == b, mb, m)
                v_new = kv_b[1, 2 * p + h]
                v3 = jnp.concatenate([v_new, v_new, v_new], axis=0)
                m = m + es.astype(BF16).astype(F32) * v3
                o = m / total
                for g in range(GROUP):
                    o_b[2 * p + h, :, g * HEAD:(g + 1) * HEAD] = o[g * 8:(g + 1) * 8].astype(BF16)

    attend(0)
    with jax.named_scope("barrier"):
        pl.semaphore_wait(barrier, greeted)

    def wd_copy(k):
        peer, j = block_peer(k)
        return pltpu.make_async_remote_copy(
            src_ref=wd.at[0, :, pl.ds(pl.multiple_of(j * NC, 128), NC)], dst_ref=wd_b.at[j_me],
            send_sem=wds_sem, recv_sem=wdr_sem, device_id=(0, peer, side), device_id_type=MESH)

    with jax.named_scope("wdsend"):
        for k in range(1, GRP):
            wd_copy(k).start()

    attend(1)

    f_copy(0).start()
    f_copy(1).start()
    wd_own.start()

    def p_copy(n):
        return pltpu.make_async_remote_copy(
            src_ref=p_own.at[n], dst_ref=p_oth.at[n], send_sem=ps_sem, recv_sem=pr_sem,
            device_id=(0, dev, other), device_id_type=MESH)

    o_all = jnp.concatenate([o_b[h] for h in range(KVH)], axis=1)

    def project(n, c):
        o_copy(n).wait()
        p_own[n] = jnp.dot(o_all, wo_b[n], preferred_element_type=F32)
        p_copy(n).start()
        return c

    with jax.named_scope("project"):
        lax.fori_loop(0, 6, project, 0)

    with jax.named_scope("x1"):
        ssq = jnp.zeros((8, 1), F32)
        pltpu.make_async_copy(p_oth, p_oth, pr_sem).wait()
        for n in range(6):
            v = hid[:, n * 512:(n + 1) * 512].astype(F32) + (p_own[n] + p_oth[n])
            v = v.astype(BF16).astype(F32)
            x1f[n] = v
            ssq = ssq + jnp.sum(v * v, axis=-1, keepdims=True)
        inv1 = lax.rsqrt(ssq / D + EPS)

        at = [ring_slot(q, cx, cy, cz) for q in range(3)]

        @pl.when(source)
        def _():
            for n in range(6):
                ring, row, col = at[n // 2]
                v = x1f[n] * inv1 * fgain[n]
                hbuf[n // 2, ring, row, col // 2, :, (n % 2) * 512:(n % 2 + 1) * 512] = v.astype(BF16)

    with jax.named_scope("ag1send"):
        @pl.when(source)
        def _():
            for i in ORDER:
                for j in ORDER:
                    if i or j:
                        for q in range(3):
                            ring, row, col = at[q]
                            block = hbuf.at[q, ring, row, col // 2]
                            pltpu.make_async_remote_copy(
                                src_ref=block, dst_ref=block, send_sem=a1s, recv_sem=a1r.at[q, (4 - i) % 4],
                                device_id=(0, chip_at(q, ring, (row + i) % 4, (col + j) % 4), side),
                                device_id_type=MESH).start()

    def recv_row(q, sem):
        some = hbuf.at[q, 0, 0]
        pltpu.make_async_copy(some, some, sem).wait()

    def own_row(g, q):
        if g == 0:
            @pl.when(source)
            def _():
                some = hbuf.at[q, 0, 0, 0]
                pltpu.make_async_copy(some, some, a1r.at[q, 0]).wait()

            @pl.when(jnp.logical_not(source))
            def _():
                recv_row(q, a1r.at[q, 0])
        else:
            recv_row(q, a1r.at[q, ORDER[g]])
        ring, row, col = at[q]
        part = hbuf.at[q, ring, (row + ORDER[g]) % 4]
        for step in (2, 1, 3):
            pltpu.make_async_remote_copy(
                src_ref=part, dst_ref=part, send_sem=a2s, recv_sem=a2r,
                device_id=(0, chip_at(q, (ring + step) % 4, row, col), side), device_id_type=MESH).start()

    for g in range(4):
        with jax.named_scope(f"own_row{g}"):
            for q in range(3):
                own_row(g, q)
    with jax.named_scope("ag2wait"):
        most = hbuf.at[:, pl.ds(0, 3)]
        pltpu.make_async_copy(most, most, a2r).wait()

    f_copy(0).wait()
    f_copy(1).wait()

    def arrange(r):
        xs = half(r)
        for i in range(8):
            y, h = i % 4, i // 4
            zs = [height(x, y, h) for x in xs]
            slots = [((xs[t], zs[t], y // 2), (y, zs[t], xs[t] // 2), (zs[t], y, xs[t] // 2)) for t in range(2)]
            for q in range(3):
                vs = [hbuf[q, ring, row, col].astype(F32) for ring, row, col in (slot[q] for slot in slots)]
                h2[r % 2, i * 16:(i + 1) * 16, q * PART:(q + 1) * PART] = jnp.concatenate(vs, axis=0).astype(BF16)

    def u_copy(k, r):
        peer, _ = block_peer(k)
        return pltpu.make_async_remote_copy(
            src_ref=ubuf.at[j_me, r], dst_ref=ubuf.at[j_me, r], send_sem=us_sem, recv_sem=ur_sem.at[r],
            device_id=(0, peer, side), device_id_type=MESH)

    for r in range(CHUNKS):
        with jax.named_scope("gateup"):
            arrange(r)
            both = jnp.dot(h2[r % 2], wgu_b[...], preferred_element_type=F32)
            gate = both[:, :FFC]
            up = both[:, FFC:]
            ubuf[j_me, r] = (gate * jax.nn.sigmoid(gate) * up).astype(BF16)
            for k in range(1, GRP):
                u_copy(k, r).start()

    wd_own.wait()
    with jax.named_scope("wdwait"):
        peers = wd_b.at[pl.ds(0, GRP - 1)]
        pltpu.make_async_copy(peers, peers, wdr_sem).wait()

    per = 64 // CHUNKS

    fx, fz = (cx + side) % 2, cz // 2

    def finish(r):
        with jax.named_scope("uwait"):
            peers = ubuf.at[pl.ds(0, GRP - 1), r]
            pltpu.make_async_copy(peers, peers, ur_sem.at[r]).wait()
        with jax.named_scope("down"):
            u_all = jnp.concatenate([ubuf[j, r] for j in range(GRP)], axis=1)
            y = jnp.dot(u_all, wd_b[...].reshape(GRP * FFC, NC), preferred_element_type=F32)
            for i in range(per // 2):
                ysend[r * per + 2 * i] = y[i * 8:i * 8 + 4]
                ysend[r * per + 2 * i + 1] = y[i * 8 + 4:i * 8 + 8]
        with jax.named_scope("give"):
            xs = half(r)
            ax, ay, az = [(a + fx) % 2 for a in range(2)], [(b + cy) % 4 for b in range(4)], [(c + fz) % 2 for c in range(2)]
            px = [jnp.where(a == 0, xs[0], xs[1]) for a in ax]
            for i in range(per):
                a, b, c, t = i % 2, (2, 1, 3, 0)[(i // 2) % 4], 1 - (i // 8) % 2, i // 16
                k = 2 * (ax[a] + 2 * ay[b] + 8 * az[c]) + t
                d = flat(px[a], ay[b], height(px[a], ay[b], az[c]))

                def start(k=k, d=d, t=t):
                    pltpu.make_async_remote_copy(
                        src_ref=ysend.at[r * per + k], dst_ref=yrecv.at[dev], send_sem=ys_sem, recv_sem=yr_sem,
                        device_id=(0, d, t), device_id_type=MESH).start()

                if r == CHUNKS - 1 and not (a or b or c):
                    pl.when(jnp.logical_not(jnp.logical_and(source, side == t)))(start)
                else:
                    start()

    for r in range(CHUNKS):
        finish(r)

    @pl.when(source)
    def _():
        yrecv[dev] = ysend[(CHUNKS - 1) * per + 2 * (fx + 2 * cy + 8 * fz) + side]

    def wait_blocks(ref, sem):
        @pl.when(source)
        def _():
            pltpu.make_async_copy(ref.at[pl.ds(0, 63)], ref.at[pl.ds(0, 63)], sem).wait()

        @pl.when(jnp.logical_not(source))
        def _():
            pltpu.make_async_copy(ref, ref, sem).wait()

    with jax.named_scope("yrwait"):
        wait_blocks(yrecv, yr_sem)
    with jax.named_scope("final"):
        x1 = jnp.concatenate([x1f[n] for n in range(6)], axis=1)
        x1 = jnp.where(side == 0, x1[0:4], x1[4:8])
        sums = []
        for j in range(GRP):
            acc = None
            for c in range(N_DEV):
                x, y, z = coords(c)
                if (x % 2) + 2 * (y % 2) + 4 * (z % 2) == j:
                    acc = yrecv[c] if acc is None else acc + yrecv[c]
            sums.append(acc)
        for j in range(GRP):
            y = jnp.where((cx + cy + cz) % 2 == 0, sums[j], sums[GRP - 1 - j])
            out[:, j * NC:(j + 1) * NC] = (x1[:, j * NC:(j + 1) * NC] + y.astype(BF16).astype(F32)).astype(BF16)

    with jax.named_scope("drain"):
        for ref, sem in ((wd_b.at[pl.ds(0, GRP - 1)], wds_sem), (ubuf.at[pl.ds(0, GRP - 1)], us_sem), (p_own, ps_sem)):
            pltpu.make_async_copy(ref, ref, sem).wait()
        @pl.when(source)
        def _():
            some = wkv_b.at[0, pl.ds(0, 3 * 15 * 16)]
            pltpu.make_async_copy(some, some, a1s).wait()

        most = hbuf.at[:, pl.ds(0, 3)]
        pltpu.make_async_copy(most, most, a2s).wait()
        wait_blocks(ysend, ys_sem)


def solution(mesh):
    batch_axes = ('inst', 'dev')
    in_specs = (
        P(batch_axes, None),
        P(batch_axes),
        P(None, batch_axes, None, None, None),
        P(None, batch_axes, None, None, None),
        P(), P(), P(), P(), P(),
        P(None, None, 'dev'),
        P(None, None, 'dev'),
        P(None, 'dev', None),
    )
    out_specs = P(('inst', 'dev', 'side'), None)
    half = HEAD // 2
    freqs = (ROPE_BASE ** (-np.arange(half, dtype=np.float64) / half)).astype(np.float32)
    freqs = np.concatenate([freqs, freqs])[None]

    def device_fn(hidden, cache_len, k_cache, v_cache, w_q, w_kv, w_o, attn_gain, ffn_gain, w_gate, w_up, w_down):
        vmem = pl.BlockSpec(memory_space=pltpu.VMEM)
        hbm = pl.BlockSpec(memory_space=pl.ANY)
        dma = pltpu.SemaphoreType.DMA
        return pl.pallas_call(
            body,
            out_shape=jax.ShapeDtypeStruct((4, D), BF16),
            in_specs=[hbm] * 13,
            out_specs=vmem,
            scratch_shapes=[
                pltpu.SMEM((8,), jnp.int32),
                pltpu.VMEM((8, D), BF16),
                pltpu.VMEM((1, D), F32),
                pltpu.VMEM((6, 1, 512), F32),
                pltpu.VMEM((1, HEAD), F32),
                pltpu.VMEM((2, D, 768), BF16),
                pltpu.VMEM((2, D, 512), BF16),
                pltpu.VMEM((6, DH, 512), BF16),
                pltpu.VMEM((2, 8, 2, SEQ, HEAD), BF16),
                pltpu.VMEM((2, 8, 2, SEQ, HEAD), BF16),
                pltpu.VMEM((D, 2 * FFC), BF16),
                pltpu.VMEM((GRP, FFC, NC), BF16),
                pltpu.VMEM((8, D), BF16),
                pltpu.VMEM((2, KVH, 8, HEAD), F32),
                pltpu.VMEM((KVH, 8, 384), BF16),
                pltpu.VMEM((6, 8, 512), F32),
                pltpu.VMEM((6, 8, 512), F32),
                pltpu.VMEM((6, 8, 512), F32),
                pltpu.VMEM((3, 4, 4, 2, 8, PART), BF16),
                pltpu.VMEM((2, CH, D), BF16),
                pltpu.VMEM((GRP, CHUNKS, CH, FFC), BF16),
                pltpu.VMEM((64, 4, NC), F32),
                pltpu.VMEM((64, 4, NC), F32),
                pltpu.VMEM((2, 8, 128), F32),
                pltpu.VMEM((24, 128), jnp.int32),
                dma((5,)), dma((2,)), dma((2,)), dma((2, 2)), dma((6,)), dma((2,)), dma, dma, dma,
                dma, dma, dma, dma((3, 4)), dma, dma, dma, dma((CHUNKS,)), dma, dma,
            ],
            compiler_params=pltpu.CompilerParams(
                collective_id=0, has_side_effects=True, vmem_limit_bytes=60 * 1024 * 1024),
            name="decode_layer",
        )(cache_len, hidden, attn_gain, ffn_gain.reshape(6, 1, 512), jnp.asarray(freqs),
          k_cache, v_cache, w_q, w_kv, w_o, w_gate, w_up, w_down)

    return jax.shard_map(device_fn, mesh=mesh, in_specs=in_specs, out_specs=out_specs, check_vma=False)
```

```python
import numpy as np
import jax
import jax.numpy as jnp
from jax import lax
from jax.experimental import pallas as pl
from jax.experimental.pallas import tpu as pltpu
from jax.sharding import PartitionSpec as P

EPS = 1e-5
ROPE_BASE = 10000.0
MESH = pl.DeviceIdType.MESH
F32 = jnp.float32
BF16 = jnp.bfloat16

N_DEV = 64
D = 3072
DH = D // 2
PART = D // 3
FFC = 128
SEQ = 256
HEAD = 128
KVH = 4
GROUP = 3
GRP = 8
NC = D // GRP
ROWS = 256
CHUNKS = 2
CH = ROWS // CHUNKS
KVC = 768
ORDER = (0, 1, 3, 2)


def coords(dev):
    return dev % 4, (dev // 4) % 4, dev // 16


def flat(x, y, z):
    return z * 16 + y * 4 + x


def ring_slot(part, x, y, z):
    return ((x, z, y), (y, z, x), (z, y, x))[part]


def chip_at(part, ring, row, col):
    return (flat(ring, col, row), flat(col, ring, row), flat(col, row, ring))[part]


def body(lens_h, hid_h, again_h, fgain_h, freq_h, kc, vc, wq, wkv, wo, wg, wu, wd, out,
         lens, hid, again, fgain, freq,
         wq_b, wkv_b, wo_b, kc_b, vc_b, wgu_b, wd_b, a_b, kv_b, o_b, p_own, p_oth, x1f,
         hbuf, h2, ubuf, ysend, yrecv, tab, lens_v,
         i_sem, w_sem, kv_sem, c_sem, wo_sem, f_sem, wd_sem, wds_sem, wdr_sem,
         ps_sem, pr_sem, a1s, a1r, a2s, a2r, us_sem, ur_sem, ys_sem, yr_sem):
    dev = lax.axis_index("dev")
    side = lax.axis_index("side")
    cx, cy, cz = coords(dev)
    j_me = (cx + side) % 2 + 2 * ((cy + side) % 2) + 4 * ((cz + side) % 2)

    source = (cx + cy + cz) % 2 == side

    def half(r):
        qx = (((cx + side) % 4) // 2 + 1 - r) % 2
        return [(2 * qx + i + 4 - side) % 4 for i in range(2)]

    def height(x, y, i):
        return 2 * i + (side + x + y) % 2

    other = 1 - side

    def in_copy(i):
        src, dst = ((hid_h, hid), (again_h, again), (fgain_h, fgain), (freq_h, freq), (lens_h, lens))[i]
        return pltpu.make_async_copy(src, dst, i_sem.at[i])

    def kv_copy(i, c):
        col = pl.multiple_of(i * 1024 + side * 512, 128)
        rows = pl.ds(c * KVC, KVC)
        return pltpu.make_async_copy(wkv.at[0, rows, pl.ds(col, 512)], wkv_b.at[i, rows], kv_sem.at[i])

    def q_copy(h):
        col = pl.multiple_of(side * DH + h * 768, 128)
        return pltpu.make_async_copy(wq.at[0, :, pl.ds(col, 768)], wq_b.at[h], w_sem.at[h])

    def c_copy(i, h):
        src, dst = (kc, kc_b) if i == 0 else (vc, vc_b)
        return pltpu.make_async_copy(src.at[0, :, pl.ds(side * KVH + 2 * h, 2)], dst.at[h], c_sem.at[i, h])

    def head_copies(h):
        q_copy(h).start()
        c_copy(0, h).start()
        c_copy(1, h).start()

    def o_copy(n):
        row = pl.multiple_of(side * DH, 128)
        return pltpu.make_async_copy(wo.at[0, pl.ds(row, DH), pl.ds(pl.multiple_of(n * 512, 128), 512)], wo_b.at[n], wo_sem.at[n])

    def f_copy(i):
        src = wg if i == 0 else wu
        return pltpu.make_async_copy(src.at[0], wgu_b.at[:, pl.ds(i * FFC, FFC)], f_sem.at[i])

    wd_own = pltpu.make_async_copy(wd.at[0, :, pl.ds(pl.multiple_of(j_me * NC, 128), NC)], wd_b.at[j_me], wd_sem)

    for i in range(5):
        in_copy(i).start()
    for c in range(D // KVC):
        kv_copy(0, c).start()

    barrier = pltpu.get_barrier_semaphore()

    def pair(c):
        return (c + 1 + 2 * ((c + side) % 2)) % 4

    def block_peer(k):
        px = pair(cx) if k % 2 else cx
        py = pair(cy) if (k // 2) % 2 else cy
        pz = pair(cz) if k // 4 else cz
        return flat(px, py, pz), (px + side) % 2 + 2 * ((py + side) % 2) + 4 * ((pz + side) % 2)

    def greet(d, t):
        pl.semaphore_signal(barrier, inc=1, device_id=(0, d, t), device_id_type=MESH)

    with jax.named_scope("greet"):
        greet(dev, other)
        greet(block_peer(GRP - 1)[0], side)
        for i in range(1, 64):
            ix, iy, iz = coords(i)
            if not (ix and iy and iz):
                greet(flat((cx + ix) % 4, (cy + iy) % 4, (cz + iz) % 4), side)
    greeted = 38

    for c in range(D // KVC):
        kv_copy(1, c).start()

    with jax.named_scope("inwait"):
        for i in range(5):
            in_copy(i).wait()

    with jax.named_scope("tables"):
        rowb = lax.broadcasted_iota(jnp.int32, (8, 128), 0)
        lv = jnp.zeros((8, 128), jnp.int32)
        for b in range(8):
            lv = jnp.where(rowb == b, lens[b], lv)
        angle = lv.astype(F32) * freq[...]
        lane = lax.broadcasted_iota(jnp.int32, (8, 128), 1)
        sin = jnp.sin(angle)
        tab[0] = jnp.cos(angle)
        tab[1] = jnp.where(lane < 64, -sin, sin)
        lens_v[...] = jnp.concatenate([lv, lv, lv], axis=0)

    def rotary(v):
        return v * tab[0] + pltpu.roll(v, 64, axis=1) * tab[1]

    with jax.named_scope("norm"):
        xf = hid[...].astype(F32)
        inv = lax.rsqrt(jnp.mean(xf * xf, axis=-1, keepdims=True) + EPS)
        a_b[...] = (xf * inv * again[...]).astype(BF16)

    for i in range(2):
        with jax.named_scope("kvwait"):
            pltpu.make_async_copy(wkv_b.at[i], wkv_b.at[i], kv_sem.at[i]).wait()
        head_copies(i)
        with jax.named_scope("kvdot"):
            kv = jnp.dot(a_b[...], wkv_b[i], preferred_element_type=F32)
            for h in range(KVH):
                v = kv[:, h * HEAD:(h + 1) * HEAD]
                if i == 0:
                    v = rotary(v)
                kv_b[i, h] = v.astype(BF16).astype(F32)

    rowm = lax.broadcasted_iota(jnp.int32, (24, SEQ), 0) % 8
    rowv = lax.broadcasted_iota(jnp.int32, (24, HEAD), 0) % 8
    pos = lax.broadcasted_iota(jnp.int32, (24, SEQ), 1)
    scale = HEAD ** -0.5

    def attend(p):
        with jax.named_scope("qwait"):
            q_copy(p).wait()
        for i in range(3):
            o_copy(3 * p + i).start()
        with jax.named_scope("qdot"):
            q = jnp.dot(a_b[...], wq_b[p], preferred_element_type=F32)
            qbs = [jnp.concatenate([rotary(q[:, (h * GROUP + g) * HEAD:(h * GROUP + g + 1) * HEAD]) for g in range(GROUP)], axis=0).astype(BF16)
                   for h in range(2)]
        with jax.named_scope("cwait"):
            c_copy(0, p).wait()
            c_copy(1, p).wait()
        with jax.named_scope("mix"):
            limit = lens_v[...]
            limit = jnp.concatenate([limit, limit], axis=1)
            scores = []
            for h in range(2):
                s = jnp.zeros((24, SEQ), F32)
                for b in range(8):
                    sb = lax.dot_general(qbs[h], kc_b[p, b, h], (((1,), (1,)), ((), ())), preferred_element_type=F32)
                    s = jnp.where(rowm == b, sb, s)
                scores.append(jnp.where(pos < limit, s * scale, -1e30))
            mixed = []
            for h in range(2):
                s = scores[h]
                k_new = kv_b[0, 2 * p + h]
                k3 = jnp.concatenate([k_new, k_new, k_new], axis=0)
                self_score = jnp.sum(qbs[h].astype(F32) * k3, axis=-1, keepdims=True) * scale
                top = jnp.maximum(jnp.max(s, axis=-1, keepdims=True), self_score)
                e = jnp.exp(s - top)
                es = jnp.exp(self_score - top)
                total = jnp.sum(e, axis=-1, keepdims=True) + es
                mixed.append((e.astype(BF16), es, total))
            for h in range(2):
                eb, es, total = mixed[h]
                m = jnp.zeros((24, HEAD), F32)
                for b in range(8):
                    mb = jnp.dot(eb, vc_b[p, b, h], preferred_element_type=F32)
                    m = jnp.where(rowv == b, mb, m)
                v_new = kv_b[1, 2 * p + h]
                v3 = jnp.concatenate([v_new, v_new, v_new], axis=0)
                m = m + es.astype(BF16).astype(F32) * v3
                o = m / total
                for g in range(GROUP):
                    o_b[2 * p + h, :, g * HEAD:(g + 1) * HEAD] = o[g * 8:(g + 1) * 8].astype(BF16)

    attend(0)
    with jax.named_scope("barrier"):
        pl.semaphore_wait(barrier, greeted)

    def wd_copy(k):
        peer, j = block_peer(k)
        return pltpu.make_async_remote_copy(
            src_ref=wd.at[0, :, pl.ds(pl.multiple_of(j * NC, 128), NC)], dst_ref=wd_b.at[j_me],
            send_sem=wds_sem, recv_sem=wdr_sem, device_id=(0, peer, side), device_id_type=MESH)

    with jax.named_scope("wdsend"):
        for k in range(1, GRP):
            wd_copy(k).start()

    attend(1)

    f_copy(0).start()
    f_copy(1).start()
    wd_own.start()

    def p_copy(n):
        return pltpu.make_async_remote_copy(
            src_ref=p_own.at[n], dst_ref=p_oth.at[n], send_sem=ps_sem, recv_sem=pr_sem,
            device_id=(0, dev, other), device_id_type=MESH)

    o_all = jnp.concatenate([o_b[h] for h in range(KVH)], axis=1)

    def project(n, c):
        o_copy(n).wait()
        p_own[n] = jnp.dot(o_all, wo_b[n], preferred_element_type=F32)
        p_copy(n).start()
        return c

    with jax.named_scope("project"):
        lax.fori_loop(0, 6, project, 0)

    with jax.named_scope("x1"):
        ssq = jnp.zeros((8, 1), F32)
        pltpu.make_async_copy(p_oth, p_oth, pr_sem).wait()
        for n in range(6):
            v = hid[:, n * 512:(n + 1) * 512].astype(F32) + (p_own[n] + p_oth[n])
            v = v.astype(BF16).astype(F32)
            x1f[n] = v
            ssq = ssq + jnp.sum(v * v, axis=-1, keepdims=True)
        inv1 = lax.rsqrt(ssq / D + EPS)

        at = [ring_slot(q, cx, cy, cz) for q in range(3)]

        @pl.when(source)
        def _():
            for n in range(6):
                ring, row, col = at[n // 2]
                v = x1f[n] * inv1 * fgain[n]
                hbuf[n // 2, ring, row, col // 2, :, (n % 2) * 512:(n % 2 + 1) * 512] = v.astype(BF16)

    with jax.named_scope("ag1send"):
        @pl.when(source)
        def _():
            for i in ORDER:
                for j in ORDER:
                    if i or j:
                        for q in range(3):
                            ring, row, col = at[q]
                            block = hbuf.at[q, ring, row, col // 2]
                            pltpu.make_async_remote_copy(
                                src_ref=block, dst_ref=block, send_sem=a1s, recv_sem=a1r.at[(4 - i) % 4],
                                device_id=(0, chip_at(q, ring, (row + i) % 4, (col + j) % 4), side),
                                device_id_type=MESH).start()

    def recv_rows(g):
        def wait(some):
            pltpu.make_async_copy(some, some, a1r.at[ORDER[g]]).wait()

        if g == 0:
            pl.when(source)(lambda: wait(hbuf.at[:, 0, 0, 0]))
            pl.when(jnp.logical_not(source))(lambda: wait(hbuf.at[:, 0, 0]))
        else:
            wait(hbuf.at[:, 0, 0])

    def own_row(g, q):
        ring, row, col = at[q]
        part = hbuf.at[q, ring, (row + ORDER[g]) % 4]
        for step in (2, 1, 3):
            pltpu.make_async_remote_copy(
                src_ref=part, dst_ref=part, send_sem=a2s, recv_sem=a2r,
                device_id=(0, chip_at(q, (ring + step) % 4, row, col), side), device_id_type=MESH).start()

    for g in range(4):
        with jax.named_scope(f"own_row{g}"):
            recv_rows(g)
            for q in range(3):
                own_row(g, q)
    with jax.named_scope("ag2wait"):
        most = hbuf.at[:, pl.ds(0, 3)]
        pltpu.make_async_copy(most, most, a2r).wait()

    f_copy(0).wait()
    f_copy(1).wait()

    def arrange(r):
        xs = half(r)
        for i in range(8):
            y, h = i % 4, i // 4
            zs = [height(x, y, h) for x in xs]
            slots = [((xs[t], zs[t], y // 2), (y, zs[t], xs[t] // 2), (zs[t], y, xs[t] // 2)) for t in range(2)]
            for q in range(3):
                vs = [hbuf[q, ring, row, col].astype(F32) for ring, row, col in (slot[q] for slot in slots)]
                h2[r % 2, i * 16:(i + 1) * 16, q * PART:(q + 1) * PART] = jnp.concatenate(vs, axis=0).astype(BF16)

    def u_copy(k, r):
        peer, _ = block_peer(k)
        return pltpu.make_async_remote_copy(
            src_ref=ubuf.at[j_me, r], dst_ref=ubuf.at[j_me, r], send_sem=us_sem, recv_sem=ur_sem.at[r],
            device_id=(0, peer, side), device_id_type=MESH)

    for r in range(CHUNKS):
        with jax.named_scope("gateup"):
            arrange(r)
            both = jnp.dot(h2[r % 2], wgu_b[...], preferred_element_type=F32)
            gate = both[:, :FFC]
            up = both[:, FFC:]
            ubuf[j_me, r] = (gate * jax.nn.sigmoid(gate) * up).astype(BF16)
            for k in range(1, GRP):
                u_copy(k, r).start()

    wd_own.wait()
    with jax.named_scope("wdwait"):
        peers = wd_b.at[pl.ds(0, GRP - 1)]
        pltpu.make_async_copy(peers, peers, wdr_sem).wait()

    per = 64 // CHUNKS

    fx, fz = (cx + side) % 2, cz // 2

    def finish(r):
        with jax.named_scope("uwait"):
            peers = ubuf.at[pl.ds(0, GRP - 1), r]
            pltpu.make_async_copy(peers, peers, ur_sem.at[r]).wait()
        with jax.named_scope("down"):
            u_all = jnp.concatenate([ubuf[j, r] for j in range(GRP)], axis=1)
            y = jnp.dot(u_all, wd_b[...].reshape(GRP * FFC, NC), preferred_element_type=F32)
            for i in range(per // 2):
                ysend[r * per + 2 * i] = y[i * 8:i * 8 + 4]
                ysend[r * per + 2 * i + 1] = y[i * 8 + 4:i * 8 + 8]
        with jax.named_scope("give"):
            xs = half(r)
            ax = [(a + fx) % 2 for a in range(2)]
            px = [jnp.where(a == 0, xs[0], xs[1]) for a in ax]
            for i in range(per):
                a, y, h, t = i % 2, (i // 2) % 4, (i // 8) % 2, i // 16
                k = 2 * (ax[a] + 2 * y + 8 * h) + t
                d = flat(px[a], y, height(px[a], y, h))

                def start(k=k, d=d, t=t):
                    pltpu.make_async_remote_copy(
                        src_ref=ysend.at[r * per + k], dst_ref=yrecv.at[dev], send_sem=ys_sem, recv_sem=yr_sem,
                        device_id=(0, d, t), device_id_type=MESH).start()

                if r == CHUNKS - 1:
                    pl.when(jnp.logical_or(d != dev, side != t))(start)
                else:
                    start()

    for r in range(CHUNKS):
        finish(r)

    @pl.when(source)
    def _():
        yrecv[dev] = ysend[(CHUNKS - 1) * per + 2 * (fx + 2 * cy + 8 * fz) + side]

    def wait_blocks(ref, sem):
        @pl.when(source)
        def _():
            pltpu.make_async_copy(ref.at[pl.ds(0, 63)], ref.at[pl.ds(0, 63)], sem).wait()

        @pl.when(jnp.logical_not(source))
        def _():
            pltpu.make_async_copy(ref, ref, sem).wait()

    with jax.named_scope("yrwait"):
        wait_blocks(yrecv, yr_sem)
    with jax.named_scope("final"):
        x1 = jnp.concatenate([x1f[n] for n in range(6)], axis=1)
        x1 = jnp.where(side == 0, x1[0:4], x1[4:8])
        sums = []
        for j in range(GRP):
            acc = None
            for c in range(N_DEV):
                x, y, z = coords(c)
                if (x % 2) + 2 * (y % 2) + 4 * (z % 2) == j:
                    acc = yrecv[c] if acc is None else acc + yrecv[c]
            sums.append(acc)
        for j in range(GRP):
            y = jnp.where((cx + cy + cz) % 2 == 0, sums[j], sums[GRP - 1 - j])
            out[:, j * NC:(j + 1) * NC] = (x1[:, j * NC:(j + 1) * NC] + y.astype(BF16).astype(F32)).astype(BF16)

    with jax.named_scope("drain"):
        for ref, sem in ((wd_b.at[pl.ds(0, GRP - 1)], wds_sem), (ubuf.at[pl.ds(0, GRP - 1)], us_sem), (p_own, ps_sem)):
            pltpu.make_async_copy(ref, ref, sem).wait()
        @pl.when(source)
        def _():
            some = wkv_b.at[0, pl.ds(0, 3 * 15 * 16)]
            pltpu.make_async_copy(some, some, a1s).wait()

        most = hbuf.at[:, pl.ds(0, 3)]
        pltpu.make_async_copy(most, most, a2s).wait()
        wait_blocks(ysend, ys_sem)


def solution(mesh):
    batch_axes = ('inst', 'dev')
    in_specs = (
        P(batch_axes, None),
        P(batch_axes),
        P(None, batch_axes, None, None, None),
        P(None, batch_axes, None, None, None),
        P(), P(), P(), P(), P(),
        P(None, None, 'dev'),
        P(None, None, 'dev'),
        P(None, 'dev', None),
    )
    out_specs = P(('inst', 'dev', 'side'), None)
    half = HEAD // 2
    freqs = (ROPE_BASE ** (-np.arange(half, dtype=np.float64) / half)).astype(np.float32)
    freqs = np.concatenate([freqs, freqs])[None]

    def device_fn(hidden, cache_len, k_cache, v_cache, w_q, w_kv, w_o, attn_gain, ffn_gain, w_gate, w_up, w_down):
        vmem = pl.BlockSpec(memory_space=pltpu.VMEM)
        hbm = pl.BlockSpec(memory_space=pl.ANY)
        dma = pltpu.SemaphoreType.DMA
        return pl.pallas_call(
            body,
            out_shape=jax.ShapeDtypeStruct((4, D), BF16),
            in_specs=[hbm] * 13,
            out_specs=vmem,
            scratch_shapes=[
                pltpu.SMEM((8,), jnp.int32),
                pltpu.VMEM((8, D), BF16),
                pltpu.VMEM((1, D), F32),
                pltpu.VMEM((6, 1, 512), F32),
                pltpu.VMEM((1, HEAD), F32),
                pltpu.VMEM((2, D, 768), BF16),
                pltpu.VMEM((2, D, 512), BF16),
                pltpu.VMEM((6, DH, 512), BF16),
                pltpu.VMEM((2, 8, 2, SEQ, HEAD), BF16),
                pltpu.VMEM((2, 8, 2, SEQ, HEAD), BF16),
                pltpu.VMEM((D, 2 * FFC), BF16),
                pltpu.VMEM((GRP, FFC, NC), BF16),
                pltpu.VMEM((8, D), BF16),
                pltpu.VMEM((2, KVH, 8, HEAD), F32),
                pltpu.VMEM((KVH, 8, 384), BF16),
                pltpu.VMEM((6, 8, 512), F32),
                pltpu.VMEM((6, 8, 512), F32),
                pltpu.VMEM((6, 8, 512), F32),
                pltpu.VMEM((3, 4, 4, 2, 8, PART), BF16),
                pltpu.VMEM((2, CH, D), BF16),
                pltpu.VMEM((GRP, CHUNKS, CH, FFC), BF16),
                pltpu.VMEM((64, 4, NC), F32),
                pltpu.VMEM((64, 4, NC), F32),
                pltpu.VMEM((2, 8, 128), F32),
                pltpu.VMEM((24, 128), jnp.int32),
                dma((5,)), dma((2,)), dma((2,)), dma((2, 2)), dma((6,)), dma((2,)), dma, dma, dma,
                dma, dma, dma, dma((4,)), dma, dma, dma, dma((CHUNKS,)), dma, dma,
            ],
            compiler_params=pltpu.CompilerParams(
                collective_id=0, has_side_effects=True, vmem_limit_bytes=60 * 1024 * 1024),
            name="decode_layer",
        )(cache_len, hidden, attn_gain, ffn_gain.reshape(6, 1, 512), jnp.asarray(freqs),
          k_cache, v_cache, w_q, w_kv, w_o, w_gate, w_up, w_down)

    return jax.shard_map(device_fn, mesh=mesh, in_specs=in_specs, out_specs=out_specs, check_vma=False)
```
